1024 devices in a mesh: gx: 8 (over y), gy: 16 (over z), gz: 8 (over x, core).
Axes of the slice: x: 4, y: 8, z: 16, core: 2. Of those that a mesh axis runs over, the one named last changes fastest.
Arguments:
- density: float32 [96, 256, 1024], P('gx', 'gy', 'gz'), may hold values from 0.5 to 8
- potential: float32 [96, 256, 1024], P('gx', 'gy', 'gz'), may hold values from -6 to 6
Outputs:
- corrected: float32 [96, 256, 1024], P('gx', 'gy', 'gz')
The draws below stay inside these ranges and needn't reach their ends.
All inputs are finite; a program needn't handle non-finite values.
Results may differ from the reference program's by a relative error of at most 0.00005.
Values sent between devices are 32-bit elements; how exact they have to be, the bound alone decides.
No kernel may reach another device: no remote copies, remote signals or barrier semaphores. Data moves between devices by JAX's collectives and lax.ppermute only.
A program may use at most 64 MiB of HBM per device.

```python
import math
import jax
import jax.numpy as jnp
from jax import lax

CX = 12
CY = 16
CZ = 128
SWEEPS = 2
NX = 96
NY = 256
NZ = 1024
N_GX = 8
N_GY = 16
N_GZ = 8


def levels(stream_key, shape, split, low, top_value):
    factor_of = 1.0
    for dim, shards_of in split:
        steps = jax.random.uniform(jax.random.fold_in(jax.random.fold_in(stream_key, 6), dim), (shards_of,), jnp.float32, low / len(split), top_value / len(split))
        factor_of = factor_of * jnp.repeat(jnp.exp(steps), shape[dim] // shards_of).reshape((-1,) + (1,) * (len(shape) - 1 - dim))
    return factor_of


def normal_values(rng, shape, width, bound, split=(), kind=jnp.bfloat16):
    level = levels(rng, shape, split, -0.22, 0.18) if split else 1.0
    entries = jax.random.normal(rng, shape, jnp.float32) * width * level
    return jnp.minimum(jnp.maximum(entries, -bound), bound).astype(kind)


def setup_inputs(seed: int = 0) -> dict:
    splits = jax.random.split(jax.random.key(seed), 3)
    return {
        "density": jnp.clip(jnp.exp(math.log(8.0) - 2.7725887 * jax.random.uniform(splits[0], (NX, NY, NZ), jnp.float32) ** levels(splits[0], (NX, NY, NZ), ((0, 8), (1, 16), (2, 8)), -0.2, 0.2)), 0.5, 8.0),
        "potential": normal_values(splits[1], (NX, NY, NZ), 1.0, 6.0, ((0, 8), (1, 16), (2, 8)), jnp.float32),
    }


def beside_all(field):
    total = jnp.roll(field, -1, 0) + jnp.roll(field, 1, 0)
    total = total + jnp.roll(field, -1, 1) + jnp.roll(field, 1, 1)
    return total + jnp.roll(field, -1, 2) + jnp.roll(field, 1, 2)

def colour(shape, offset):
    summed = lax.broadcasted_iota(jnp.int32, shape, 0) + lax.broadcasted_iota(jnp.int32, shape, 1)
    summed = summed + lax.broadcasted_iota(jnp.int32, shape, 2) + offset
    return summed % 2 == 0

def smooth(field, source, red):
    field = jnp.where(red, (beside_all(field) - source) / 6.0, field)
    return jnp.where(red, field, (beside_all(field) - source) / 6.0)

def basis(count):
    rows = lax.broadcasted_iota(jnp.int32, (count, count), 0).astype(jnp.float32)
    cols = lax.broadcasted_iota(jnp.int32, (count, count), 1)
    freq = ((cols + 1) // 2).astype(jnp.float32)
    angle = 2.0 * jnp.pi * freq * rows / count
    full = jnp.sqrt(2.0 / count)
    single = 1.0 / jnp.sqrt(jnp.float32(count))
    top = 2 * ((cols + 1) // 2) == count
    table = jnp.where(cols % 2 == 1, jnp.cos(angle) * full, jnp.sin(angle) * full)
    table = jnp.where(top, jnp.cos(angle) * single, table)
    table = jnp.where(cols == 0, single, table)
    modes = ((jnp.arange(count, dtype=jnp.int32) + 1) // 2).astype(jnp.float32)
    return (table, 2.0 - 2.0 * jnp.cos(2.0 * jnp.pi * modes / count))

def coarse_solve(blocks, weight_x, weight_y, weight_z):
    nx, ny, nz = blocks.shape
    qx, lx = basis(nx)
    qy, ly = basis(ny)
    qz, lz = basis(nz)
    hi = lax.Precision.HIGHEST
    spectrum = jnp.einsum('ia,jb,kc,ijk->abc', qx, qy, qz, blocks, precision=hi)
    denom = weight_x * lx[:, None, None] + weight_y * ly[None, :, None] + weight_z * lz[None, None, :]
    zero = colour((nx, ny, nz), 0) & (lax.broadcasted_iota(jnp.int32, (nx, ny, nz), 0) + lax.broadcasted_iota(jnp.int32, (nx, ny, nz), 1) + lax.broadcasted_iota(jnp.int32, (nx, ny, nz), 2) == 0)
    safe = jnp.where(zero, jnp.float32(1.0), denom)
    spectrum = jnp.where(zero, jnp.float32(0.0), -spectrum / safe)
    return jnp.einsum('ia,jb,kc,abc->ijk', qx, qy, qz, spectrum, precision=hi)

def widen(field, bx, by, bz):
    return jnp.repeat(jnp.repeat(jnp.repeat(field, bx, 0), by, 1), bz, 2)

def reference(density, potential):
    source = density - jnp.sum(density) / (NX * NY * NZ)
    red = colour(source.shape, 0)
    fine = potential
    for sweep in range(SWEEPS):
        fine = smooth(fine, source, red)
    left = source - (beside_all(fine) - 6.0 * fine)
    level_one = left.reshape(NX // 2, 2, NY // 2, 2, NZ // 2, 2).sum(axis=(1, 3, 5)) * 0.5
    red_one = colour(level_one.shape, 0)
    error_one = jnp.zeros_like(level_one)
    for sweep in range(SWEEPS):
        error_one = smooth(error_one, level_one, red_one)
    rest = level_one - (beside_all(error_one) - 6.0 * error_one)
    bx, by, bz = (CX // 2, CY // 2, CZ // 2)
    blocks = rest.reshape(N_GX, bx, N_GY, by, N_GZ, bz).sum(axis=(1, 3, 5))
    coarse = coarse_solve(blocks, float(by * bz), float(bx * bz), float(bx * by))
    error_one = error_one + widen(coarse, bx, by, bz)
    for sweep in range(SWEEPS):
        error_one = smooth(error_one, level_one, red_one)
    fine = fine + widen(error_one, 2, 2, 2)
    for sweep in range(SWEEPS):
        fine = smooth(fine, source, red)
    return fine
```

```python
import functools

import jax
import jax.numpy as jnp
import numpy as np
from jax import lax
from jax.experimental import pallas as pl
from jax.experimental.pallas import tpu as pltpu
from jax.sharding import PartitionSpec as P

GX, GY, GZ = 8, 16, 8
BX, BY, BZ = 6, 8, 64
LANES = 128
SHIFT = 4.25
SIXTH = 1.0 / 6.0
HI = lax.Precision.HIGHEST
F32 = jnp.float32


def roll(x, shift, axis):
    return pltpu.roll(x, shift % x.shape[axis], axis)


def iota(shape, dim):
    return lax.broadcasted_iota(jnp.int32, shape, dim)


def dot(a, b):
    return lax.dot_general(a, b, (((1,), (0,)), ((), ())), precision=HI, preferred_element_type=F32)


def dot_nt(a, b):
    return lax.dot_general(a, b, (((1,), (1,)), ((), ())), precision=HI, preferred_element_type=F32)


def plus(a, b):
    if a is None:
        return b
    return a if b is None else a + b


def basis_of(count):
    rows = np.arange(count)[:, None]
    cols = np.arange(count)[None, :]
    freq = (cols + 1) // 2
    angle = 2.0 * np.pi * freq * rows / count
    table = np.where(cols % 2 == 1, np.cos(angle), np.sin(angle)) * np.sqrt(2.0 / count)
    table = np.where(2 * freq == count, np.cos(angle) / np.sqrt(count), table)
    table = np.where(cols == 0, 1.0 / np.sqrt(count), table)
    modes = (np.arange(count) + 1) // 2
    return table, 2.0 - 2.0 * np.cos(2.0 * np.pi * modes / count)


def coarse_tables():
    qx, lx = basis_of(GX)
    qy, ly = basis_of(GY)
    qz, lz = basis_of(GZ)
    qyz = np.einsum("jb,kc->jkbc", qy, qz).reshape(LANES, LANES)
    lam = BY * BZ * lx[:, None, None] + BX * BZ * ly[None, :, None] + BX * BY * lz[None, None, :]
    lam[0, 0, 0] = 1.0
    inverse = -1.0 / lam
    inverse[0, 0, 0] = 0.0
    inverse = inverse.reshape(GX, LANES)
    around = lambda n: np.arange(-1, n + 1) % n
    tx = np.repeat(qx[around(GX)][:, :, None], LANES, axis=2)
    ty = np.repeat(qy[around(GY)], GZ, axis=1)
    tz = np.tile(qz[around(GZ)], (1, GY))
    return [np.asarray(t, np.float32) for t in (qyz, inverse, tx, ty, tz)]


def parting():
    table = np.zeros((LANES, LANES), np.float32)
    for z in range(LANES):
        table[z, (z % 2) * 64 + z // 2] = 1.0
    return table


def unit_response():
    red = black = 0.0
    for _ in range(2):
        red = (6 * black - 1) / 6
        black = (6 * red - 1) / 6
    level = 0.5 * (4 * (1 - (6 * black - 6 * red)) + 4 * (1 - (6 * red - 6 * black)))
    one = [0.0, 0.0]
    for _ in range(4):
        one[0] = (6 * one[1] - level) / 6
        one[1] = (6 * one[0] - level) / 6
    v = [[own + group for own in (red, black)] for group in one]
    for _ in range(2):
        for own in (0, 1):
            near = 3 * (v[0][1 - own] + v[1][1 - own])
            v[0][own] = v[1][own] = (near - 1) / 6
    return v


CELLS = [(a, b, c) for a in (0, 1) for b in (0, 1) for c in (0, 1)]


def spread(depth, a, count):
    low = -((depth + a) // 2)
    high = (2 * count + depth - 1 - a) // 2
    return range(low, high + 1)


def beside(field, cell, x):
    a, b, c = cell
    total = plus(field.get(((1 - a, b, c), x)), field.get(((1 - a, b, c), x + (1 if a else -1))))
    other = field.get(((a, 1 - b, c), x))
    if other is not None:
        total = plus(total, other + roll(other, -1 if b else 1, 0))
    other = field.get(((a, b, 1 - c), x))
    if other is not None:
        total = plus(total, other + roll(other, -1 if c else 1, 1))
    return total


class Kept:
    def __init__(self, ref):
        self.ref = ref
        self.slots = {}

    def get(self, key):
        slot = self.slots.get(key)
        return None if slot is None else self.ref[slot]

    def put(self, key, value):
        slot = self.slots.setdefault(key, len(self.slots))
        self.ref[slot] = value


def fine_half(field, source, colour, depth):
    for cell in CELLS:
        if sum(cell) % 2 != colour:
            continue
        for x in spread(depth, cell[0], BX):
            near = beside(field, cell, x)
            s = source.get((cell, x))
            if near is None and s is None:
                continue
            value = near if s is None else (-s if near is None else near - s)
            field.put((cell, x), value * SIXTH)


def coarsened(field, source, x):
    total = None
    for cell in CELLS:
        if sum(cell) % 2 != 0:
            continue
        near = beside(field, cell, x)
        s = source.get((cell, x))
        own = field.get((cell, x))
        part = None if own is None else 6.0 * own
        part = plus(part, s)
        if near is not None:
            part = -near if part is None else part - near
        total = plus(total, part)
    return None if total is None else total * 0.5


def red_of(shape, x):
    return (iota(shape, 0) + iota(shape, 1) + (x % 2)) % 2 == 0


def beside_one(field, x):
    total = plus(field.get(x - 1), field.get(x + 1))
    own = field.get(x)
    if own is not None:
        total = plus(total, roll(own, 1, 0) + roll(own, -1, 0))
        total = total + (roll(own, 1, 1) + roll(own, -1, 1))
    return total


def one_half(field, source, colour, low, high, masks):
    for x in range(low, high):
        near = beside_one(field, x)
        s = source.get(x)
        own = field.get(x)
        if near is None and s is None:
            continue
        value = near if s is None else (-s if near is None else near - s)
        value = value * SIXTH
        red = masks[x % 2]
        rest = jnp.zeros_like(value) if own is None else own
        field.put(x, jnp.where(red, value, rest) if colour == 0 else jnp.where(red, rest, value))


def part_kernel(density, potential, table, out, dscratch, pscratch):
    t = table[...]
    dscratch[...] = dot(density[...].reshape(192, LANES) - SHIFT, t)
    pscratch[...] = dot(potential[...].reshape(192, LANES), t)
    low = iota((BY, LANES), 1) < 64
    for x in range(BX):
        for a in (0, 1):
            rows = []
            for b in (0, 1):
                at = pl.ds((2 * x + a) * 16 + b, BY, stride=2)
                out[2 * a + b, x] = dscratch[at, :]
                rows.append(pscratch[at, :])
            out[4 + a, x] = jnp.where(low, rows[1 - a], rows[a])


def source_slot(cell):
    return 2 * cell[0] + cell[1]


def halves(cell):
    return 4 + cell[0], cell[2]


def share_kernel(pairs, out, fref, sref, eref, lref, stack):
    own = iota((BY, LANES), 1) < 64
    source, field = Kept(sref), Kept(fref)
    nothing = jnp.zeros((BY, LANES), F32)
    mass = None
    for cell in CELLS:
        for x in range(BX):
            value = pairs[source_slot(cell), x]
            mass = plus(mass, value) if cell[2] == 0 else mass
            if cell[2]:
                value = roll(value, 64, 1)
            source.put((cell, x), jnp.concatenate([jnp.where(own, value, 0.0), nothing], 0))
            if sum(cell) % 2:
                array, half = halves(cell)
                value = pairs[array, x]
                if half:
                    value = roll(value, 64, 1)
                field.put((cell, x), jnp.concatenate([jnp.where(own, value, 0.0), nothing], 0))
    for step in range(4):
        fine_half(field, source, step % 2, step + 1)
    level, error = Kept(lref), Kept(eref)
    near = iota((BY, LANES), 0) < 4
    for x in range(-3, BX + 3):
        value = coarsened(field, source, x)
        top, rim = value[:BY], value[BY:]
        level.put(x, jnp.concatenate([top, jnp.where(near, rim, 0.0), jnp.where(near, 0.0, rim)], 0))
    masks = [red_of((24, LANES), x) for x in (0, 1)]
    for step in range(4):
        one_half(error, level, step % 2, -3 - step, BX + 3 + step, masks)
    for i, (low, high) in enumerate(((-7, -6), (-6, 0), (0, 6), (6, 12), (12, 13))):
        total = None
        for x in range(low, high):
            part = plus(level.get(x), None if error.get(x) is None else 6.0 * error.get(x))
            around = beside_one(error, x)
            part = -around if part is None else part - around
            total = plus(total, jnp.where(masks[x % 2], part, 0.0))
        for j in range(3):
            stack[pl.ds((3 * i + j) * 8, 8), :] = total[8 * j : 8 * j + 8]
    stack[pl.ds(120, 8), :] = mass
    rows, cols = iota((LANES, LANES), 0), iota((LANES, LANES), 1)
    summed = dot(jnp.where(cols // 8 == rows, 1.0, 0.0), stack[...])
    row, lane = iota((8, LANES), 0), iota((8, LANES), 1)
    pick = ((row == 0) & (lane < 64)) | ((row == 1) & (lane >= 64) & (lane < 96))
    pick = pick | ((row == 2) & (lane >= 96))
    summed = jnp.where((rows == 15) & (cols < 64), summed + roll(summed, 64, 1), summed)
    summed = jnp.where((rows == 15) & (cols >= 64), 0.0, summed)
    sent = dot_nt(jnp.where(pick, 1.0, 0.0), summed)
    for peer in range(GZ):
        out[peer] = sent


def along_z_kernel(got, out):
    total = got[:, 0, :] + roll(got[:, 1, :], 1, 0) + roll(got[:, 2, :], -1, 0)
    rows, cols = iota((LANES, LANES), 0), iota((LANES, LANES), 1)
    tiled = dot(total, jnp.where((rows < 16) & (cols % 16 == rows), 1.0, 0.0))
    row, lane = iota((GZ, LANES), 0), iota((GZ, LANES), 1)
    flat = jnp.sum(jnp.where(lane // 16 == row, tiled, 0.0), axis=0, keepdims=True)
    for peer in range(GY):
        out[peer] = flat


def along_y_kernel(got, out):
    values = got[:, 0, :]
    slot = iota((GY, LANES), 1) % 16
    total = jnp.where((slot % 3 == 0) | (slot == 15), values, 0.0)
    total = total + roll(jnp.where((slot % 3 == 1), values, 0.0), 1, 0)
    total = total + roll(jnp.where((slot % 3 == 2), values, 0.0), -1, 0)
    rows, cols = iota((LANES, LANES), 0), iota((LANES, LANES), 1)
    row, lane = iota((GY, LANES), 0), iota((GY, LANES), 1)
    place = iota((8, LANES), 0)
    sent = jnp.zeros((8, LANES), F32)
    for r in range(6):
        take = (cols % 8 == rows // 16) & ((rows % 16) // 3 == r)
        tiled = dot(total, jnp.where(take, 1.0, 0.0))
        flat = jnp.sum(jnp.where(lane // 8 == row, tiled, 0.0), axis=0, keepdims=True)
        sent = jnp.where(place == r, flat, sent)
    for peer in range(GX):
        out[peer] = sent


def wide_x(own, left, right, array, x):
    if x < 0:
        return left[array, x + BX]
    if x >= BX:
        return right[array, x - BX]
    return own[array, x]


def rim_y_kernel(own, left, right, low, high):
    for array in range(6):
        for x in range(-BX, 2 * BX):
            value = wide_x(own, left, right, array, x)
            low[array, x + BX] = value[:4]
            high[array, x + BX] = value[4:]


def tall(own, left, right, below, above, array, x):
    value = wide_x(own, left, right, array, x)
    rim = jnp.concatenate([above[array, x + BX], below[array, x + BX]], 0)
    return jnp.concatenate([value, rim], 0)


def groups():
    made = []
    for x in range(-BX, 2 * BX):
        made.append((x + BX, [(i, x) for i in range(4)]))
    for x in range(-BX, 3):
        made.append((18 + x + BX, [(4, x), (5, x), (4, x + 9), (5, x + 9)]))
    return made


def rim_z_kernel(own, left, right, below, above, low, high):
    lane = iota((16, LANES), 1)
    for slot, members in groups():
        lows = highs = None
        for i, (array, x) in enumerate(members):
            value = tall(own, left, right, below, above, array, x)
            down = roll(value, 16 * i, 1)
            up = roll(value, 16 * (i + 1), 1)
            lows = down if lows is None else jnp.where((lane % 64) // 16 == i, down, lows)
            highs = up if highs is None else jnp.where((lane % 64) // 16 == i, up, highs)
        low[slot] = lows
        high[slot] = highs


def fine_kernel(own, left, right, below, above, before, after, level, fine, kept, fref, sref):
    source, field = Kept(sref), Kept(fref)
    lane = iota((16, LANES), 1)
    home = {}
    for slot, members in groups():
        for i, key in enumerate(members):
            home[key] = (slot, i)
    for array in range(6):
        for x in range(-BX, 2 * BX):
            value = tall(own, left, right, below, above, array, x)
            slot, i = home[(array, x)]
            up, down = after[slot], before[slot]
            for c in (0, 1):
                mine = roll(value, 64, 1) if c else value
                right_rim = roll(up, 64 - 16 * i - 64 * c, 1)
                left_rim = roll(down, 48 - 16 * i + 64 * c, 1)
                full = jnp.where(lane < 64, mine, 0.0)
                full = jnp.where((lane >= 64) & (lane < 80), right_rim, full)
                full = jnp.where(lane >= 112, left_rim, full)
                if array < 4:
                    source.put(((array // 2, array % 2, c), x), full)
                else:
                    a = array - 4
                    b = (1 + a + c) % 2
                    field.put(((a, b, c), x), full)
    for step, depth in enumerate((10, 9, 8, 7)):
        fine_half(field, source, step % 2, depth)
    for x in range(-3, BX + 3):
        level[x + 3] = coarsened(field, source, x)
    for n, cell in enumerate(CELLS):
        for x in range(-2, BX + 2):
            fine[n, x + 2] = field.get((cell, x))
            kept[n, x + 2] = source.get((cell, x))


def level_y_kernel(own, below, above, wide, low, high):
    first = iota((8, LANES), 0) == 0
    last = iota((8, LANES), 0) == 7
    for x in range(12):
        mine, down, up = own[x], below[x], above[x]
        tail = jnp.where(first, up[8:16], 0.0)
        lead = jnp.where(last, down[8:16], 0.0)
        value = jnp.concatenate([mine[:8], up[:8], tail + lead, down[:8]], 0)
        wide[x] = value
        if x >= 3:
            low[x - 3] = value
        if x < 9:
            high[x] = value


def mid_kernel(wide, left, right, level, mid, eref):
    for x in range(-9, BX + 9):
        if x < 0:
            value = left[x + 9]
        elif x >= BX:
            value = right[x - BX]
        else:
            value = wide[x + 3]
        level[x + 9] = value
    source = Given(level, 9, 24)
    error = Kept(eref)
    masks = [red_of((32, LANES), x) for x in (0, 1)]
    for step, depth in enumerate((9, 8, 7, 6)):
        one_half(error, source, step % 2, -depth, BX + depth, masks)
    for x in range(-6, BX + 6):
        mid[x + 6] = error.get(x)


class Given:
    def __init__(self, ref, start, count):
        self.ref, self.start, self.count = ref, start, count

    def get(self, x):
        return self.ref[x + self.start] if 0 <= x + self.start < self.count else None

    def put(self, x, value):
        self.ref[x + self.start] = value


def last_kernel(got, qyz, inverse, tx, ty, tz, level, mid, fine, kept, table, out, eref, fref, oref, *, axes):
    blocks = None
    for r in range(5):
        blocks = plus(blocks, roll(got[:, r, :], r - 2, 0))
    mean = jnp.sum(got[:, 5, :], keepdims=True) * (1.0 / (GX * GY * GZ * 8 * BX * BY * BZ))
    blocks = blocks - jnp.sum(blocks, keepdims=True) * (1.0 / (GX * GY * GZ))
    half = dot(blocks, qyz[...])
    modes = None
    for x in range(GX):
        modes = plus(modes, half[x : x + 1, :] * tx[x + 1])
    modes = modes * inverse[...]
    ix, iy, iz = axes
    own_lane = iota((LANES, LANES), 0)
    zrow = lambda d: tz[pl.ds(iz + 1 + d, 1), :]
    spread_z = jnp.where(own_lane < 64, zrow(0), jnp.where(own_lane < 96, zrow(1), zrow(-1)))
    place = iota((16, LANES), 0)
    stacked = jnp.zeros((16, LANES), F32)
    for dx in (-1, 0, 1):
        line = jnp.sum(modes * tx[ix + 1 + dx], axis=0, keepdims=True)
        for dy in (-1, 0, 1):
            stacked = jnp.where(place == 3 * (dx + 1) + dy + 1, line * ty[pl.ds(iy + 1 + dy, 1), :], stacked)
    coarse = dot_nt(stacked, spread_z)
    row = iota((32, LANES), 0)
    error = Given(eref, 6, 18)
    for dx in (-1, 0, 1):
        r = 3 * (dx + 1)
        add = jnp.where(row < 8, coarse[r + 1 : r + 2], jnp.where(row < 16, coarse[r + 2 : r + 3], coarse[r : r + 1]))
        for x in range(BX * dx, BX * dx + BX):
            error.put(x, mid[x + 6] + add)
    source = Given(level, 9, 24)
    masks = [red_of((32, LANES), x) for x in (0, 1)]
    for step, depth in enumerate((5, 4, 3, 2)):
        one_half(error, source, step % 2, -depth, BX + depth, masks)
    near = iota((8, LANES), 0) < 4
    field, terms = Kept(fref), Sources(kept)
    for x in range(-2, BX + 2):
        e = error.get(x)
        e = jnp.concatenate([e[:8], jnp.where(near, e[8:16], e[24:])], 0)
        for n, cell in enumerate(CELLS):
            field.put((cell, x), fine[n, x + 2] + e)
    for step, depth in enumerate((3, 2, 1, 0)):
        fine_half(field, terms, step % 2, depth)
    v = unit_response()
    shape = (8, LANES)
    lane = iota(shape, 1)
    for x in range(BX):
        group = (iota(shape, 0) + lane + x) % 2 == 0
        for a in (0, 1):
            for b in (0, 1):
                pair = []
                for c in (0, 1):
                    own = (a + b + c) % 2
                    value = field.get(((a, b, c), x))[:8]
                    pair.append(value - mean * jnp.where(group, v[0][own], v[1][own]))
                both = jnp.where(lane < 64, pair[0], roll(pair[1], 64, 1))
                oref[pl.ds((2 * x + a) * 16 + b, 8, stride=2), :] = both
    out[...] = dot_nt(oref[...], table[...]).reshape(12, 16, LANES)


class Sources:
    def __init__(self, ref):
        self.ref = ref

    def get(self, key):
        cell, x = key
        return self.ref[CELLS.index(cell), x + 2] if -2 <= x < BX + 2 else None


def run(kernel, shapes, args, scratch=(), flops=1000000, **static):
    space = pl.BlockSpec(memory_space=pltpu.VMEM)
    moved = 4 * sum(int(np.prod(s)) for s in shapes)
    return pl.pallas_call(
        kernel,
        out_shape=[jax.ShapeDtypeStruct(s, F32) for s in shapes],
        in_specs=[space] * len(args),
        out_specs=[space] * len(shapes),
        scratch_shapes=[pltpu.VMEM(s, F32) for s in scratch],
        cost_estimate=pl.CostEstimate(flops=flops, bytes_accessed=moved, transcendentals=0),
        name=kernel.__name__,
    )(*args)


def place_kernel(*refs):
    axes = (lax.axis_index("gx"), lax.axis_index("gy"), lax.axis_index("gz"))
    last_kernel(*refs, axes=axes)


def moved(array, axis, step):
    count = lax.axis_size(axis)
    return lax.ppermute(array, axis, [(i, (i + step) % count) for i in range(count)])


def everyone(array, axis):
    return lax.all_to_all(array, axis, 0, 0, tiled=True)


def body(density, potential):
    qyz, inverse, tx, ty, tz = (jnp.asarray(t) for t in coarse_tables())
    table = jnp.asarray(parting())
    (own,) = run(part_kernel, [(6, 6, 8, LANES)], [density, potential, table], [(192, LANES)] * 2)
    left, right = moved(own, "gx", 1), moved(own, "gx", -1)
    (shares,) = run(
        share_kernel,
        [(GZ, 8, LANES)],
        [own],
        [(96, 16, LANES), (48, 16, LANES), (20, 24, LANES), (12, 24, LANES), (LANES, LANES)],
    )
    (line,) = run(along_z_kernel, [(GY, 1, LANES)], [everyone(shares, "gz")])
    (plane,) = run(along_y_kernel, [(GX, 8, LANES)], [everyone(line, "gy")])
    blocks = everyone(plane, "gx")
    low, high = run(rim_y_kernel, [(6, 18, 4, LANES)] * 2, [own, left, right])
    below, above = moved(high, "gy", 1), moved(low, "gy", -1)
    low, high = run(rim_z_kernel, [(27, 16, LANES)] * 2, [own, left, right, below, above])
    before, after = moved(high, "gz", 1), moved(low, "gz", -1)
    level, fine, kept = run(
        fine_kernel,
        [(12, 16, LANES), (8, 10, 16, LANES), (8, 10, 16, LANES)],
        [own, left, right, below, above, before, after],
        [(144, 16, LANES), (144, 16, LANES)],
    )
    below, above = moved(level, "gy", 1), moved(level, "gy", -1)
    wide, low, high = run(
        level_y_kernel, [(12, 32, LANES), (9, 32, LANES), (9, 32, LANES)], [level, below, above]
    )
    left, right = moved(high, "gx", 1), moved(low, "gx", -1)
    level, mid = run(
        mid_kernel, [(24, 32, LANES), (18, 32, LANES)], [wide, left, right], [(24, 32, LANES)]
    )
    (out,) = run(
        place_kernel,
        [(12, 16, LANES)],
        [blocks, qyz, inverse, tx, ty, tz, level, mid, fine, kept, table],
        [(18, 32, LANES), (80, 16, LANES), (192, LANES)],
    )
    return out


def solution(mesh):
    spec = P("gx", "gy", "gz")
    return jax.shard_map(body, mesh=mesh, in_specs=(spec, spec), out_specs=spec, check_vma=False)
```

```python
import jax
import jax.numpy as jnp
import numpy as np
from jax import lax
from jax.experimental import pallas as pl
from jax.experimental.pallas import tpu as pltpu
from jax.sharding import PartitionSpec as P


GX, GY, GZ = 8, 16, 8
BX, BY, BZ = 6, 8, 64
LANES = 128
SHIFT = 4.25
SIXTH = 1.0 / 6.0
HI = lax.Precision.HIGHEST
F32 = jnp.float32


def roll(x, shift, axis):
    return pltpu.roll(x, shift % x.shape[axis], axis)


def iota(shape, dim):
    return lax.broadcasted_iota(jnp.int32, shape, dim)


def dot(a, b):
    return lax.dot_general(a, b, (((1,), (0,)), ((), ())), precision=HI, preferred_element_type=F32)


def dot_nt(a, b):
    return lax.dot_general(a, b, (((1,), (1,)), ((), ())), precision=HI, preferred_element_type=F32)


def plus(a, b):
    if a is None:
        return b
    return a if b is None else a + b


def basis_of(count):
    rows = np.arange(count)[:, None]
    cols = np.arange(count)[None, :]
    freq = (cols + 1) // 2
    angle = 2.0 * np.pi * freq * rows / count
    table = np.where(cols % 2 == 1, np.cos(angle), np.sin(angle)) * np.sqrt(2.0 / count)
    table = np.where(2 * freq == count, np.cos(angle) / np.sqrt(count), table)
    table = np.where(cols == 0, 1.0 / np.sqrt(count), table)
    modes = (np.arange(count) + 1) // 2
    return table, 2.0 - 2.0 * np.cos(2.0 * np.pi * modes / count)


def coarse_tables():
    qx, lx = basis_of(GX)
    qy, ly = basis_of(GY)
    qz, lz = basis_of(GZ)
    count = GX * GZ
    qxz = np.zeros((LANES, LANES))
    qxz[:count, :count] = np.einsum("ia,kc->ikac", qx, qz).reshape(count, count)
    lam = BX * BZ * ly[:, None, None] + BY * BZ * lx[None, :, None] + BX * BY * lz[None, None, :]
    lam[0, 0, 0] = 1.0
    table = -1.0 / lam
    table[0, 0, 0] = 0.0
    inverse = np.zeros((GY, LANES))
    inverse[:, :count] = table.reshape(GY, count)
    around = lambda n: np.arange(-1, n + 1) % n
    ty = np.repeat(qy[around(GY)][:, :, None], LANES, axis=2)
    tx = np.zeros((GX + 2, LANES))
    tx[:, :count] = np.repeat(qx[around(GX)], GZ, axis=1)
    tz = np.zeros((GZ + 2, LANES))
    tz[:, :count] = np.tile(qz[around(GZ)], (1, GX))
    return [np.asarray(t, np.float32) for t in (qxz, inverse, tx, ty, tz)]


def parting():
    table = np.zeros((LANES, LANES), np.float32)
    for z in range(LANES):
        table[z, (z % 2) * 64 + z // 2] = 1.0
    return table


def unit_response():
    red = black = 0.0
    for _ in range(2):
        red = (6 * black - 1) / 6
        black = (6 * red - 1) / 6
    level = 0.5 * (4 * (1 - (6 * black - 6 * red)) + 4 * (1 - (6 * red - 6 * black)))
    one = [0.0, 0.0]
    for _ in range(4):
        one[0] = (6 * one[1] - level) / 6
        one[1] = (6 * one[0] - level) / 6
    v = [[own + group for own in (red, black)] for group in one]
    for _ in range(2):
        for own in (0, 1):
            near = 3 * (v[0][1 - own] + v[1][1 - own])
            v[0][own] = v[1][own] = (near - 1) / 6
    return v


CELLS = [(a, b, c) for a in (0, 1) for b in (0, 1) for c in (0, 1)]


def spread(depth, a, count):
    low = -((depth + a) // 2)
    high = (2 * count + depth - 1 - a) // 2
    return range(low, high + 1)


def beside(field, cell, x):
    a, b, c = cell
    total = plus(field.get(((1 - a, b, c), x)), field.get(((1 - a, b, c), x + (1 if a else -1))))
    other = field.get(((a, 1 - b, c), x))
    if other is not None:
        total = plus(total, other + roll(other, -1 if b else 1, 0))
    other = field.get(((a, b, 1 - c), x))
    if other is not None:
        total = plus(total, other + roll(other, -1 if c else 1, 1))
    return total


class Kept:
    def __init__(self, ref):
        self.ref = ref
        self.slots = {}

    def get(self, key):
        slot = self.slots.get(key)
        return None if slot is None else self.ref[slot]

    def put(self, key, value):
        slot = self.slots.setdefault(key, len(self.slots))
        self.ref[slot] = value


def fine_half(field, source, colour, depth):
    for cell in CELLS:
        if sum(cell) % 2 != colour:
            continue
        for x in spread(depth, cell[0], BX):
            near = beside(field, cell, x)
            s = source.get((cell, x))
            if near is None and s is None:
                continue
            value = near if s is None else (-s if near is None else near - s)
            field.put((cell, x), value * SIXTH)


def coarsened(field, source, x):
    total = None
    for cell in CELLS:
        if sum(cell) % 2 != 0:
            continue
        near = beside(field, cell, x)
        s = source.get((cell, x))
        own = field.get((cell, x))
        part = None if own is None else 6.0 * own
        part = plus(part, s)
        if near is not None:
            part = -near if part is None else part - near
        total = plus(total, part)
    return None if total is None else total * 0.5


def red_of(shape, x):
    return (iota(shape, 0) + iota(shape, 1) + (x % 2)) % 2 == 0


def beside_one(field, x):
    total = plus(field.get(x - 1), field.get(x + 1))
    own = field.get(x)
    if own is not None:
        total = plus(total, roll(own, 1, 0) + roll(own, -1, 0))
        total = total + (roll(own, 1, 1) + roll(own, -1, 1))
    return total


def one_half(field, source, colour, low, high, masks):
    for x in range(low, high):
        near = beside_one(field, x)
        s = source.get(x)
        own = field.get(x)
        if near is None and s is None:
            continue
        value = near if s is None else (-s if near is None else near - s)
        value = value * SIXTH
        red = masks[x % 2]
        rest = jnp.zeros_like(value) if own is None else own
        field.put(x, jnp.where(red, value, rest) if colour == 0 else jnp.where(red, rest, value))


def part_kernel(density, potential, table, out, dscratch, pscratch):
    t = table[...]
    dscratch[...] = dot(density[...].reshape(192, LANES) - SHIFT, t)
    pscratch[...] = dot(potential[...].reshape(192, LANES), t)
    low = iota((BY, LANES), 1) < 64
    for x in range(BX):
        for a in (0, 1):
            rows = []
            for b in (0, 1):
                at = pl.ds((2 * x + a) * 16 + b, BY, stride=2)
                out[2 * a + b, x] = dscratch[at, :]
                rows.append(pscratch[at, :])
            out[4 + a, x] = jnp.where(low, rows[1 - a], rows[a])


def source_slot(cell):
    return 2 * cell[0] + cell[1]


def halves(cell):
    return 4 + cell[0], cell[2]


def share_kernel(pairs, out, fref, sref, eref, lref, stack):
    own = iota((BY, LANES), 1) < 64
    source, field = Kept(sref), Kept(fref)
    nothing = jnp.zeros((BY, LANES), F32)
    mass = None
    for cell in CELLS:
        for x in range(BX):
            value = pairs[source_slot(cell), x]
            mass = plus(mass, value) if cell[2] == 0 else mass
            if cell[2]:
                value = roll(value, 64, 1)
            source.put((cell, x), jnp.concatenate([jnp.where(own, value, 0.0), nothing], 0))
            if sum(cell) % 2:
                array, half = halves(cell)
                value = pairs[array, x]
                if half:
                    value = roll(value, 64, 1)
                field.put((cell, x), jnp.concatenate([jnp.where(own, value, 0.0), nothing], 0))
    for step in range(4):
        fine_half(field, source, step % 2, step + 1)
    level, error = Kept(lref), Kept(eref)
    near = iota((BY, LANES), 0) < 4
    for x in range(-3, BX + 3):
        value = coarsened(field, source, x)
        top, rim = value[:BY], value[BY:]
        level.put(x, jnp.concatenate([top, jnp.where(near, rim, 0.0), jnp.where(near, 0.0, rim)], 0))
    masks = [red_of((24, LANES), x) for x in (0, 1)]
    for step in range(4):
        one_half(error, level, step % 2, -3 - step, BX + 3 + step, masks)
    for i, (low, high) in enumerate(((-7, -6), (-6, 0), (0, 6), (6, 12), (12, 13))):
        total = None
        for x in range(low, high):
            part = plus(level.get(x), None if error.get(x) is None else 6.0 * error.get(x))
            around = beside_one(error, x)
            part = -around if part is None else part - around
            total = plus(total, jnp.where(masks[x % 2], part, 0.0))
        for j in range(3):
            stack[pl.ds((3 * i + j) * 8, 8), :] = total[8 * j : 8 * j + 8]
    stack[pl.ds(120, 8), :] = mass
    rows, cols = iota((LANES, LANES), 0), iota((LANES, LANES), 1)
    summed = dot(jnp.where(cols // 8 == rows, 1.0, 0.0), stack[...])
    row, lane = iota((8, LANES), 0), iota((8, LANES), 1)
    pick = ((row == 0) & (lane < 64)) | ((row == 1) & (lane >= 64) & (lane < 96))
    pick = pick | ((row == 2) & (lane >= 96))
    summed = jnp.where((rows == 15) & (cols < 64), summed + roll(summed, 64, 1), summed)
    summed = jnp.where((rows == 15) & (cols >= 64), 0.0, summed)
    sent = dot_nt(jnp.where(pick, 1.0, 0.0), summed)
    flat = sent[0:1] + roll(sent[1:2], 16, 1) + roll(sent[2:3], 32, 1)
    for peer in range(GX * GZ):
        out[peer] = flat


def along_xz_kernel(got, out):
    values = got[:, 0, :]
    lane = iota((GZ, LANES), 1)
    part, slot = lane // 16, lane % 16
    lines = []
    for i in range(GX):
        line = values[GZ * i : GZ * i + GZ]
        total = jnp.where(part == 0, line, 0.0)
        total = total + roll(jnp.where(part == 1, line, 0.0), 1, 0)
        lines.append(total + roll(jnp.where(part == 2, line, 0.0), -1, 0))
    rows = []
    for i in range(GX):
        total = jnp.where(slot == 15, lines[i], 0.0)
        for r in range(5):
            total = jnp.where((slot < 15) & (slot // 3 == r), lines[(i - (r - 2)) % GX], total)
        rows.append(total)
    total = jnp.concatenate(rows + rows, 0)
    row, col = iota((8, LANES), 0), iota((8, LANES), 1)
    take = (col < 48) & (col % 16 < 15) & ((col % 16) % 3 == row)
    take = take | ((row == 3) & (col == 15))
    sums = dot_nt(jnp.where(take, 1.0, 0.0), total)
    first = iota((1, LANES), 1) < 64
    sent = [jnp.where(first, sums[0:1], sums[1:2]), jnp.where(first, sums[2:3], sums[3:4])]
    sent = jnp.concatenate(sent, 0)
    for peer in range(GY):
        out[peer] = sent


def sides(axis, first, second):
    odd = lax.axis_index(axis) % 2 == 1

    def pick(swap):
        return lambda *at: jnp.where(odd != swap, first[at], second[at])

    return pick(False), pick(True)


def for_swaps(axis, low, high):
    odd = lax.axis_index(axis) % 2 == 1
    return jnp.where(odd, low, high), jnp.where(odd, high, low)


def wide_x(own, left, right, array, x):
    if x < 0:
        return left(array, x + BX)
    if x >= BX:
        return right(array, x - BX)
    return own[array, x]


def rim_y_kernel(own, xa, xb, ya, yb):
    left, right = sides("gx", xa, xb)
    for array in range(6):
        for x in range(-BX, 2 * BX):
            value = wide_x(own, left, right, array, x)
            ya[array, x + BX], yb[array, x + BX] = for_swaps("gy", value[:4], value[4:])


def tall(own, left, right, below, above, array, x):
    value = wide_x(own, left, right, array, x)
    rim = jnp.concatenate([above(array, x + BX), below(array, x + BX)], 0)
    return jnp.concatenate([value, rim], 0)


def groups():
    made = []
    for x in range(-BX, 2 * BX):
        made.append((x + BX, [(i, x) for i in range(4)]))
    for x in range(-BX, 3):
        made.append((18 + x + BX, [(4, x), (5, x), (4, x + 9), (5, x + 9)]))
    return made


def rim_z_kernel(own, xa, xb, ya, yb, za, zb):
    left, right = sides("gx", xa, xb)
    below, above = sides("gy", ya, yb)
    lane = iota((16, LANES), 1)
    for slot, members in groups():
        lows = highs = None
        for i, (array, x) in enumerate(members):
            value = tall(own, left, right, below, above, array, x)
            down = roll(value, 16 * i, 1)
            up = roll(value, 16 * (i + 1), 1)
            lows = down if lows is None else jnp.where((lane % 64) // 16 == i, down, lows)
            highs = up if highs is None else jnp.where((lane % 64) // 16 == i, up, highs)
        za[slot], zb[slot] = for_swaps("gz", lows, highs)


def fine_kernel(own, xa, xb, ya, yb, za, zb, level, fine, kept, fref, sref):
    left, right = sides("gx", xa, xb)
    below, above = sides("gy", ya, yb)
    before, after = sides("gz", za, zb)
    source, field = Kept(sref), Kept(fref)
    lane = iota((16, LANES), 1)
    home = {}
    for slot, members in groups():
        for i, key in enumerate(members):
            home[key] = (slot, i)
    for array in range(6):
        for x in range(-BX, 2 * BX):
            value = tall(own, left, right, below, above, array, x)
            slot, i = home[(array, x)]
            up, down = after(slot), before(slot)
            for c in (0, 1):
                mine = roll(value, 64, 1) if c else value
                right_rim = roll(up, 64 - 16 * i - 64 * c, 1)
                left_rim = roll(down, 48 - 16 * i + 64 * c, 1)
                full = jnp.where(lane < 64, mine, 0.0)
                full = jnp.where((lane >= 64) & (lane < 80), right_rim, full)
                full = jnp.where(lane >= 112, left_rim, full)
                if array < 4:
                    source.put(((array // 2, array % 2, c), x), full)
                else:
                    a = array - 4
                    b = (1 + a + c) % 2
                    field.put(((a, b, c), x), full)
    for step, depth in enumerate((10, 9, 8, 7)):
        fine_half(field, source, step % 2, depth)
    for x in range(-3, BX + 3):
        level[x + 3] = coarsened(field, source, x)
    for n, cell in enumerate(CELLS):
        for x in range(-2, BX + 2):
            fine[n, x + 2] = field.get((cell, x))
            kept[n, x + 2] = source.get((cell, x))


def level_y_kernel(own, ya, yb, wide, xa, xb):
    below, above = sides("gy", ya, yb)
    first = iota((8, LANES), 0) == 0
    last = iota((8, LANES), 0) == 7
    for x in range(12):
        mine, down, up = own[x], below(x), above(x)
        tail = jnp.where(first, up[8:16], 0.0)
        lead = jnp.where(last, down[8:16], 0.0)
        value = jnp.concatenate([mine[:8], up[:8], tail + lead, down[:8]], 0)
        wide[x] = value
    for x in range(9):
        xa[x], xb[x] = for_swaps("gx", wide[x + 3], wide[x])


def mid_kernel(wide, xa, xb, level, mid, eref):
    left, right = sides("gx", xa, xb)
    for x in range(-9, BX + 9):
        if x < 0:
            value = left(x + 9)
        elif x >= BX:
            value = right(x - BX)
        else:
            value = wide[x + 3]
        level[x + 9] = value
    source = Given(level, 9, 24)
    error = Kept(eref)
    masks = [red_of((32, LANES), x) for x in (0, 1)]
    for step, depth in enumerate((9, 8, 7, 6)):
        one_half(error, source, step % 2, -depth, BX + depth, masks)
    for x in range(-6, BX + 6):
        mid[x + 6] = error.get(x)


class Given:
    def __init__(self, ref, start, count):
        self.ref, self.start, self.count = ref, start, count

    def get(self, x):
        return self.ref[x + self.start] if 0 <= x + self.start < self.count else None

    def put(self, x, value):
        self.ref[x + self.start] = value


def last_kernel(got, qxz, inverse, tx, ty, tz, level, mid, fine, kept, table, out, eref, fref, oref, *, axes):
    one, two = got[:, 0, :], got[:, 1, :]
    blocks = one + roll(roll(one, 64, 1), 1, 0) + roll(two, -1, 0)
    inside = iota((GY, LANES), 1) < GX * GZ
    mean = jnp.sum(jnp.where(inside, 0.0, two), keepdims=True)
    mean = mean * (1.0 / (GX * GY * GZ * 8 * BX * BY * BZ))
    blocks = jnp.where(inside, blocks, 0.0)
    level_out = jnp.sum(blocks, keepdims=True) * (1.0 / (GX * GY * GZ))
    blocks = jnp.where(inside, blocks - level_out, 0.0)
    half = dot(blocks, qxz[...])
    modes = None
    for y in range(GY):
        modes = plus(modes, half[y : y + 1, :] * ty[y + 1])
    modes = modes * inverse[...]
    ix, iy, iz = axes
    own_lane = iota((LANES, LANES), 0)
    zrow = lambda d: tz[pl.ds(iz + 1 + d, 1), :]
    spread_z = jnp.where(own_lane < 64, zrow(0), jnp.where(own_lane < 96, zrow(1), zrow(-1)))
    place = iota((16, LANES), 0)
    stacked = jnp.zeros((16, LANES), F32)
    for dy in (-1, 0, 1):
        line = jnp.sum(modes * ty[iy + 1 + dy], axis=0, keepdims=True)
        for dx in (-1, 0, 1):
            both = line * tx[pl.ds(ix + 1 + dx, 1), :]
            stacked = jnp.where(place == 3 * (dx + 1) + dy + 1, both, stacked)
    coarse = dot_nt(stacked, spread_z)
    row = iota((32, LANES), 0)
    error = Given(eref, 6, 18)
    for dx in (-1, 0, 1):
        r = 3 * (dx + 1)
        add = jnp.where(row < 8, coarse[r + 1 : r + 2], jnp.where(row < 16, coarse[r + 2 : r + 3], coarse[r : r + 1]))
        for x in range(BX * dx, BX * dx + BX):
            error.put(x, mid[x + 6] + add)
    source = Given(level, 9, 24)
    masks = [red_of((32, LANES), x) for x in (0, 1)]
    for step, depth in enumerate((5, 4, 3, 2)):
        one_half(error, source, step % 2, -depth, BX + depth, masks)
    near = iota((8, LANES), 0) < 4
    field, terms = Kept(fref), Sources(kept)
    for x in range(-2, BX + 2):
        e = error.get(x)
        e = jnp.concatenate([e[:8], jnp.where(near, e[8:16], e[24:])], 0)
        for n, cell in enumerate(CELLS):
            field.put((cell, x), fine[n, x + 2] + e)
    for step, depth in enumerate((3, 2, 1, 0)):
        fine_half(field, terms, step % 2, depth)
    v = unit_response()
    shape = (8, LANES)
    lane = iota(shape, 1)
    for x in range(BX):
        group = (iota(shape, 0) + lane + x) % 2 == 0
        for a in (0, 1):
            for b in (0, 1):
                pair = []
                for c in (0, 1):
                    own = (a + b + c) % 2
                    value = field.get(((a, b, c), x))[:8]
                    pair.append(value - mean * jnp.where(group, v[0][own], v[1][own]))
                both = jnp.where(lane < 64, pair[0], roll(pair[1], 64, 1))
                oref[pl.ds((2 * x + a) * 16 + b, 8, stride=2), :] = both
    out[...] = dot_nt(oref[...], table[...]).reshape(12, 16, LANES)


class Sources:
    def __init__(self, ref):
        self.ref = ref

    def get(self, key):
        cell, x = key
        return self.ref[CELLS.index(cell), x + 2] if -2 <= x < BX + 2 else None


def run(kernel, shapes, args, scratch=(), flops=500000000):
    space = pl.BlockSpec(memory_space=pltpu.VMEM)
    moved = 4 * sum(int(np.prod(s)) for s in shapes)
    return pl.pallas_call(
        kernel,
        out_shape=[jax.ShapeDtypeStruct(s, F32) for s in shapes],
        in_specs=[space] * len(args),
        out_specs=[space] * len(shapes),
        scratch_shapes=[pltpu.VMEM(s, F32) for s in scratch],
        cost_estimate=pl.CostEstimate(flops=flops, bytes_accessed=moved, transcendentals=0),
        compiler_params=pltpu.CompilerParams(vmem_limit_bytes=16 << 20),
    )(*args)


def place_kernel(*refs):
    axes = (lax.axis_index("gx"), lax.axis_index("gy"), lax.axis_index("gz"))
    last_kernel(*refs, axes=axes)


def swapped(first, second, axis):
    count = lax.axis_size(axis)
    one = [(i, i ^ 1) for i in range(count)]
    two = [(i, (i + 1 if i % 2 else i - 1) % count) for i in range(count)]
    got = lax.ppermute(first, axis, one)
    return got, lax.ppermute(second, axis, two)


def everyone(array, axis):
    return lax.all_to_all(array, axis, 0, 0, tiled=True)


def steps(density, potential):
    tables = [jnp.asarray(t) for t in coarse_tables()]
    table = jnp.asarray(parting())
    (own,) = run(part_kernel, [(6, 6, 8, LANES)], [density, potential, table], [(192, LANES)] * 2)
    xs = swapped(own, own, "gx")
    (shares,) = run(
        share_kernel,
        [(GX * GZ, 1, LANES)],
        [own],
        [(96, 16, LANES), (48, 16, LANES), (20, 24, LANES), (12, 24, LANES), (LANES, LANES)],
    )
    (plane,) = run(along_xz_kernel, [(GY, 2, LANES)], [everyone(shares, ("gx", "gz"))])
    blocks = everyone(plane, "gy")
    ys = swapped(*run(rim_y_kernel, [(6, 18, 4, LANES)] * 2, [own, *xs]), "gy")
    zs = swapped(*run(rim_z_kernel, [(27, 16, LANES)] * 2, [own, *xs, *ys]), "gz")
    level, fine, kept = run(
        fine_kernel,
        [(12, 16, LANES), (8, 10, 16, LANES), (8, 10, 16, LANES)],
        [own, *xs, *ys, *zs],
        [(144, 16, LANES), (144, 16, LANES)],
    )
    ys = swapped(level, level, "gy")
    wide, xa, xb = run(
        level_y_kernel, [(12, 32, LANES), (9, 32, LANES), (9, 32, LANES)], [level, *ys]
    )
    xs = swapped(xa, xb, "gx")
    level, mid = run(
        mid_kernel, [(24, 32, LANES), (18, 32, LANES)], [wide, *xs], [(24, 32, LANES)]
    )
    (out,) = run(
        place_kernel,
        [(12, 16, LANES)],
        [blocks, *tables, level, mid, fine, kept, table],
        [(18, 32, LANES), (80, 16, LANES), (192, LANES)],
    )
    return out


def solution(mesh):
    spec = P("gx", "gy", "gz")
    return jax.shard_map(steps, mesh=mesh, in_specs=(spec, spec), out_specs=spec, check_vma=False)
```

```python
import jax
import jax.numpy as jnp
import numpy as np
from jax import lax
from jax.experimental import pallas as pl
from jax.experimental.pallas import tpu as pltpu
from jax.sharding import PartitionSpec as P


GX, GY, GZ = 8, 16, 8
BX, BY, BZ = 6, 8, 64
LANES = 128
SHIFT = 4.25
SIXTH = 1.0 / 6.0
HI = lax.Precision.HIGHEST
F32 = jnp.float32


def roll(x, shift, axis):
    return pltpu.roll(x, shift % x.shape[axis], axis)


def iota(shape, dim):
    return lax.broadcasted_iota(jnp.int32, shape, dim)


def dot(a, b):
    return lax.dot_general(a, b, (((1,), (0,)), ((), ())), precision=HI, preferred_element_type=F32)


def dot_nt(a, b):
    return lax.dot_general(a, b, (((1,), (1,)), ((), ())), precision=HI, preferred_element_type=F32)


def plus(a, b):
    if a is None:
        return b
    return a if b is None else a + b


def basis_of(count):
    rows = np.arange(count)[:, None]
    cols = np.arange(count)[None, :]
    freq = (cols + 1) // 2
    angle = 2.0 * np.pi * freq * rows / count
    table = np.where(cols % 2 == 1, np.cos(angle), np.sin(angle)) * np.sqrt(2.0 / count)
    table = np.where(2 * freq == count, np.cos(angle) / np.sqrt(count), table)
    table = np.where(cols == 0, 1.0 / np.sqrt(count), table)
    modes = (np.arange(count) + 1) // 2
    return table, 2.0 - 2.0 * np.cos(2.0 * np.pi * modes / count)


def coarse_tables():
    qx, lx = basis_of(GX)
    qy, ly = basis_of(GY)
    qz, lz = basis_of(GZ)
    count = GX * GZ
    qxz = np.zeros((LANES, LANES))
    qxz[:count, :count] = np.einsum("ia,kc->ikac", qx, qz).reshape(count, count)
    lam = BX * BZ * ly[:, None, None] + BY * BZ * lx[None, :, None] + BX * BY * lz[None, None, :]
    lam[0, 0, 0] = 1.0
    table = -1.0 / lam
    table[0, 0, 0] = 0.0
    inverse = np.zeros((GY, LANES))
    inverse[:, :count] = table.reshape(GY, count)
    around = lambda n: np.arange(-1, n + 1) % n
    ty = np.repeat(qy[around(GY)][:, :, None], LANES, axis=2)
    tx = np.zeros((GX + 2, LANES))
    tx[:, :count] = np.repeat(qx[around(GX)], GZ, axis=1)
    tz = np.zeros((GZ + 2, LANES))
    tz[:, :count] = np.tile(qz[around(GZ)], (1, GX))
    return [np.asarray(t, np.float32) for t in (qxz, inverse, tx, ty, tz)]


def parting():
    rows, cols = iota((LANES, LANES), 0), iota((LANES, LANES), 1)
    return jnp.where(cols == (rows % 2) * 64 + rows // 2, 1.0, 0.0)


def unit_response():
    red = black = 0.0
    for _ in range(2):
        red = (6 * black - 1) / 6
        black = (6 * red - 1) / 6
    level = 0.5 * (4 * (1 - (6 * black - 6 * red)) + 4 * (1 - (6 * red - 6 * black)))
    one = [0.0, 0.0]
    for _ in range(4):
        one[0] = (6 * one[1] - level) / 6
        one[1] = (6 * one[0] - level) / 6
    v = [[own + group for own in (red, black)] for group in one]
    for _ in range(2):
        for own in (0, 1):
            near = 3 * (v[0][1 - own] + v[1][1 - own])
            v[0][own] = v[1][own] = (near - 1) / 6
    return v


CELLS = [(a, b, c) for a in (0, 1) for b in (0, 1) for c in (0, 1)]


def spread(depth, a, count):
    low = -((depth + a) // 2)
    high = (2 * count + depth - 1 - a) // 2
    return range(low, high + 1)


def beside(field, cell, x):
    a, b, c = cell
    total = plus(field.get(((1 - a, b, c), x)), field.get(((1 - a, b, c), x + (1 if a else -1))))
    other = field.get(((a, 1 - b, c), x))
    if other is not None:
        total = plus(total, other + roll(other, -1 if b else 1, 0))
    other = field.get(((a, b, 1 - c), x))
    if other is not None:
        total = plus(total, other + roll(other, -1 if c else 1, 1))
    return total


class Kept:
    def __init__(self, ref):
        self.ref = ref
        self.slots = {}

    def get(self, key):
        slot = self.slots.get(key)
        return None if slot is None else self.ref[slot]

    def put(self, key, value):
        slot = self.slots.setdefault(key, len(self.slots))
        self.ref[slot] = value


def fine_half(field, source, colour, depth):
    for cell in CELLS:
        if sum(cell) % 2 != colour:
            continue
        for x in spread(depth, cell[0], BX):
            near = beside(field, cell, x)
            s = source.get((cell, x))
            if near is None and s is None:
                continue
            value = near if s is None else (-s if near is None else near - s)
            field.put((cell, x), value * SIXTH)


def coarsened(field, source, x):
    total = None
    for cell in CELLS:
        if sum(cell) % 2 != 0:
            continue
        near = beside(field, cell, x)
        s = source.get((cell, x))
        own = field.get((cell, x))
        part = None if own is None else 6.0 * own
        part = plus(part, s)
        if near is not None:
            part = -near if part is None else part - near
        total = plus(total, part)
    return None if total is None else total * 0.5


def red_of(shape, x):
    return (iota(shape, 0) + iota(shape, 1) + (x % 2)) % 2 == 0


def beside_one(field, x):
    total = plus(field.get(x - 1), field.get(x + 1))
    own = field.get(x)
    if own is not None:
        total = plus(total, roll(own, 1, 0) + roll(own, -1, 0))
        total = total + (roll(own, 1, 1) + roll(own, -1, 1))
    return total


def one_half(field, source, colour, low, high, masks):
    for x in range(low, high):
        near = beside_one(field, x)
        s = source.get(x)
        own = field.get(x)
        if near is None and s is None:
            continue
        value = near if s is None else (-s if near is None else near - s)
        value = value * SIXTH
        red = masks[x % 2]
        rest = jnp.zeros_like(value) if own is None else own
        field.put(x, jnp.where(red, value, rest) if colour == 0 else jnp.where(red, rest, value))


def part_kernel(density, potential, out, dscratch, pscratch):
    t = parting()
    dscratch[...] = dot(density[...].reshape(192, LANES) - SHIFT, t)
    pscratch[...] = dot(potential[...].reshape(192, LANES), t)
    low = iota((BY, LANES), 1) < 64
    for x in range(BX):
        for a in (0, 1):
            rows = []
            for b in (0, 1):
                at = pl.ds((2 * x + a) * 16 + b, BY, stride=2)
                out[2 * a + b, x] = dscratch[at, :]
                rows.append(pscratch[at, :])
            out[4 + a, x] = jnp.where(low, rows[1 - a], rows[a])


def source_slot(cell):
    return 2 * cell[0] + cell[1]


def halves(cell):
    return 4 + cell[0], cell[2]


def share_kernel(pairs, out, fref, sref, eref, lref, stack):
    own = iota((BY, LANES), 1) < 64
    source, field = Kept(sref), Kept(fref)
    nothing = jnp.zeros((BY, LANES), F32)
    mass = None
    for cell in CELLS:
        for x in range(BX):
            value = pairs[source_slot(cell), x]
            mass = plus(mass, value) if cell[2] == 0 else mass
            if cell[2]:
                value = roll(value, 64, 1)
            source.put((cell, x), jnp.concatenate([jnp.where(own, value, 0.0), nothing], 0))
            if sum(cell) % 2:
                array, half = halves(cell)
                value = pairs[array, x]
                if half:
                    value = roll(value, 64, 1)
                field.put((cell, x), jnp.concatenate([jnp.where(own, value, 0.0), nothing], 0))
    for step in range(4):
        fine_half(field, source, step % 2, step + 1)
    level, error = Kept(lref), Kept(eref)
    near = iota((BY, LANES), 0) < 4
    for x in range(-3, BX + 3):
        value = coarsened(field, source, x)
        top, rim = value[:BY], value[BY:]
        level.put(x, jnp.concatenate([top, jnp.where(near, rim, 0.0), jnp.where(near, 0.0, rim)], 0))
    masks = [red_of((24, LANES), x) for x in (0, 1)]
    for step in range(4):
        one_half(error, level, step % 2, -3 - step, BX + 3 + step, masks)
    for i, (low, high) in enumerate(((-7, -6), (-6, 0), (0, 6), (6, 12), (12, 13))):
        total = None
        for x in range(low, high):
            part = plus(level.get(x), None if error.get(x) is None else 6.0 * error.get(x))
            around = beside_one(error, x)
            part = -around if part is None else part - around
            total = plus(total, jnp.where(masks[x % 2], part, 0.0))
        for j in range(3):
            stack[pl.ds((3 * i + j) * 8, 8), :] = total[8 * j : 8 * j + 8]
    stack[pl.ds(120, 8), :] = mass
    rows, cols = iota((LANES, LANES), 0), iota((LANES, LANES), 1)
    summed = dot(jnp.where(cols // 8 == rows, 1.0, 0.0), stack[...])
    row, lane = iota((8, LANES), 0), iota((8, LANES), 1)
    pick = ((row == 0) & (lane < 64)) | ((row == 1) & (lane >= 64) & (lane < 96))
    pick = pick | ((row == 2) & (lane >= 96))
    summed = jnp.where((rows == 15) & (cols < 64), summed + roll(summed, 64, 1), summed)
    summed = jnp.where((rows == 15) & (cols >= 64), 0.0, summed)
    sent = dot_nt(jnp.where(pick, 1.0, 0.0), summed)
    flat = sent[0:1] + roll(sent[1:2], 16, 1) + roll(sent[2:3], 32, 1)
    for peer in range(GX * GZ):
        out[peer] = flat


def along_xz_kernel(got, out):
    values = got[:, 0, :]
    lane = iota((GZ, LANES), 1)
    part, slot = lane // 16, lane % 16
    lines = []
    for i in range(GX):
        line = values[GZ * i : GZ * i + GZ]
        total = jnp.where(part == 0, line, 0.0)
        total = total + roll(jnp.where(part == 1, line, 0.0), 1, 0)
        lines.append(total + roll(jnp.where(part == 2, line, 0.0), -1, 0))
    rows = []
    for i in range(GX):
        total = jnp.where(slot == 15, lines[i], 0.0)
        for r in range(5):
            total = jnp.where((slot < 15) & (slot // 3 == r), lines[(i - (r - 2)) % GX], total)
        rows.append(total)
    total = jnp.concatenate(rows + rows, 0)
    row, col = iota((8, LANES), 0), iota((8, LANES), 1)
    take = (col < 48) & (col % 16 < 15) & ((col % 16) % 3 == row)
    take = take | ((row == 3) & (col == 15))
    sums = dot_nt(jnp.where(take, 1.0, 0.0), total)
    first = iota((1, LANES), 1) < 64
    sent = [jnp.where(first, sums[0:1], sums[1:2]), jnp.where(first, sums[2:3], sums[3:4])]
    sent = jnp.concatenate(sent, 0)
    for peer in range(GY):
        out[peer] = sent


def sides(axis, first, second):
    odd = lax.axis_index(axis) % 2 == 1

    def pick(swap):
        return lambda *at: jnp.where(odd != swap, first[at], second[at])

    return pick(False), pick(True)


def for_swaps(axis, low, high):
    odd = lax.axis_index(axis) % 2 == 1
    return jnp.where(odd, low, high), jnp.where(odd, high, low)


def wide_x(own, left, right, array, x):
    if x < 0:
        return left(array, x + BX)
    if x >= BX:
        return right(array, x - BX)
    return own[array, x]


def rim_y_kernel(own, xa, xb, ya, yb):
    left, right = sides("gx", xa, xb)
    for array in range(6):
        for x in range(-BX, 2 * BX):
            value = wide_x(own, left, right, array, x)
            ya[array, x + BX], yb[array, x + BX] = for_swaps("gy", value[:4], value[4:])


def tall(own, left, right, below, above, array, x):
    value = wide_x(own, left, right, array, x)
    rim = jnp.concatenate([above(array, x + BX), below(array, x + BX)], 0)
    return jnp.concatenate([value, rim], 0)


def groups():
    made = []
    for x in range(-BX, 2 * BX):
        made.append((x + BX, [(i, x) for i in range(4)]))
    for x in range(-BX, 3):
        made.append((18 + x + BX, [(4, x), (5, x), (4, x + 9), (5, x + 9)]))
    return made


def rim_z_kernel(own, xa, xb, ya, yb, za, zb):
    left, right = sides("gx", xa, xb)
    below, above = sides("gy", ya, yb)
    lane = iota((16, LANES), 1)
    for slot, members in groups():
        lows = highs = None
        for i, (array, x) in enumerate(members):
            value = tall(own, left, right, below, above, array, x)
            down = roll(value, 16 * i, 1)
            up = roll(value, 16 * (i + 1), 1)
            lows = down if lows is None else jnp.where((lane % 64) // 16 == i, down, lows)
            highs = up if highs is None else jnp.where((lane % 64) // 16 == i, up, highs)
        za[slot], zb[slot] = for_swaps("gz", lows, highs)


def fine_kernel(own, xa, xb, ya, yb, za, zb, level, fine, kept, fref, sref):
    left, right = sides("gx", xa, xb)
    below, above = sides("gy", ya, yb)
    before, after = sides("gz", za, zb)
    source, field = Kept(sref), Kept(fref)
    lane = iota((16, LANES), 1)
    home = {}
    for slot, members in groups():
        for i, key in enumerate(members):
            home[key] = (slot, i)
    for array in range(6):
        for x in range(-BX, 2 * BX):
            value = tall(own, left, right, below, above, array, x)
            slot, i = home[(array, x)]
            up, down = after(slot), before(slot)
            for c in (0, 1):
                mine = roll(value, 64, 1) if c else value
                right_rim = roll(up, 64 - 16 * i - 64 * c, 1)
                left_rim = roll(down, 48 - 16 * i + 64 * c, 1)
                full = jnp.where(lane < 64, mine, 0.0)
                full = jnp.where((lane >= 64) & (lane < 80), right_rim, full)
                full = jnp.where(lane >= 112, left_rim, full)
                if array < 4:
                    source.put(((array // 2, array % 2, c), x), full)
                else:
                    a = array - 4
                    b = (1 + a + c) % 2
                    field.put(((a, b, c), x), full)
    for step, depth in enumerate((10, 9, 8, 7)):
        fine_half(field, source, step % 2, depth)
    for x in range(-3, BX + 3):
        level[x + 3] = coarsened(field, source, x)
    for n, cell in enumerate(CELLS):
        for x in range(-2, BX + 2):
            fine[n, x + 2] = field.get((cell, x))
            kept[n, x + 2] = source.get((cell, x))


def level_y_kernel(own, ya, yb, wide, xa, xb):
    below, above = sides("gy", ya, yb)
    first = iota((8, LANES), 0) == 0
    last = iota((8, LANES), 0) == 7
    for x in range(12):
        mine, down, up = own[x], below(x), above(x)
        tail = jnp.where(first, up[8:16], 0.0)
        lead = jnp.where(last, down[8:16], 0.0)
        value = jnp.concatenate([mine[:8], up[:8], tail + lead, down[:8]], 0)
        wide[x] = value
    for x in range(9):
        xa[x], xb[x] = for_swaps("gx", wide[x + 3], wide[x])


def mid_kernel(wide, xa, xb, level, mid, eref):
    left, right = sides("gx", xa, xb)
    for x in range(-9, BX + 9):
        if x < 0:
            value = left(x + 9)
        elif x >= BX:
            value = right(x - BX)
        else:
            value = wide[x + 3]
        level[x + 9] = value
    source = Given(level, 9, 24)
    error = Kept(eref)
    masks = [red_of((32, LANES), x) for x in (0, 1)]
    for step, depth in enumerate((9, 8, 7, 6)):
        one_half(error, source, step % 2, -depth, BX + depth, masks)
    for x in range(-6, BX + 6):
        mid[x + 6] = error.get(x)


class Given:
    def __init__(self, ref, start, count):
        self.ref, self.start, self.count = ref, start, count

    def get(self, x):
        return self.ref[x + self.start] if 0 <= x + self.start < self.count else None

    def put(self, x, value):
        self.ref[x + self.start] = value


def last_kernel(got, qxz, inverse, tx, ty, tz, level, mid, fine, kept, out, eref, fref, oref, *, axes):
    one, two = got[:, 0, :], got[:, 1, :]
    blocks = one + roll(roll(one, 64, 1), 1, 0) + roll(two, -1, 0)
    inside = iota((GY, LANES), 1) < GX * GZ
    mean = jnp.sum(jnp.where(inside, 0.0, two), keepdims=True)
    mean = mean * (1.0 / (GX * GY * GZ * 8 * BX * BY * BZ))
    blocks = jnp.where(inside, blocks, 0.0)
    level_out = jnp.sum(blocks, keepdims=True) * (1.0 / (GX * GY * GZ))
    blocks = jnp.where(inside, blocks - level_out, 0.0)
    half = dot(blocks, qxz[...])
    modes = None
    for y in range(GY):
        modes = plus(modes, half[y : y + 1, :] * ty[y + 1])
    modes = modes * inverse[...]
    ix, iy, iz = axes
    own_lane = iota((LANES, LANES), 0)
    zrow = lambda d: tz[pl.ds(iz + 1 + d, 1), :]
    spread_z = jnp.where(own_lane < 64, zrow(0), jnp.where(own_lane < 96, zrow(1), zrow(-1)))
    place = iota((16, LANES), 0)
    stacked = jnp.zeros((16, LANES), F32)
    for dy in (-1, 0, 1):
        line = jnp.sum(modes * ty[iy + 1 + dy], axis=0, keepdims=True)
        for dx in (-1, 0, 1):
            both = line * tx[pl.ds(ix + 1 + dx, 1), :]
            stacked = jnp.where(place == 3 * (dx + 1) + dy + 1, both, stacked)
    coarse = dot_nt(stacked, spread_z)
    row = iota((32, LANES), 0)
    error = Given(eref, 6, 18)
    for dx in (-1, 0, 1):
        r = 3 * (dx + 1)
        add = jnp.where(row < 8, coarse[r + 1 : r + 2], jnp.where(row < 16, coarse[r + 2 : r + 3], coarse[r : r + 1]))
        for x in range(BX * dx, BX * dx + BX):
            error.put(x, mid[x + 6] + add)
    source = Given(level, 9, 24)
    masks = [red_of((32, LANES), x) for x in (0, 1)]
    for step, depth in enumerate((5, 4, 3, 2)):
        one_half(error, source, step % 2, -depth, BX + depth, masks)
    near = iota((8, LANES), 0) < 4
    field, terms = Kept(fref), Sources(kept)
    for x in range(-2, BX + 2):
        e = error.get(x)
        e = jnp.concatenate([e[:8], jnp.where(near, e[8:16], e[24:])], 0)
        for n, cell in enumerate(CELLS):
            field.put((cell, x), fine[n, x + 2] + e)
    for step, depth in enumerate((3, 2, 1, 0)):
        fine_half(field, terms, step % 2, depth)
    v = unit_response()
    shape = (8, LANES)
    lane = iota(shape, 1)
    for x in range(BX):
        group = (iota(shape, 0) + lane + x) % 2 == 0
        for a in (0, 1):
            for b in (0, 1):
                pair = []
                for c in (0, 1):
                    own = (a + b + c) % 2
                    value = field.get(((a, b, c), x))[:8]
                    pair.append(value - mean * jnp.where(group, v[0][own], v[1][own]))
                both = jnp.where(lane < 64, pair[0], roll(pair[1], 64, 1))
                oref[pl.ds((2 * x + a) * 16 + b, 8, stride=2), :] = both
    out[...] = dot_nt(oref[...], parting()).reshape(12, 16, LANES)


class Sources:
    def __init__(self, ref):
        self.ref = ref

    def get(self, key):
        cell, x = key
        return self.ref[CELLS.index(cell), x + 2] if -2 <= x < BX + 2 else None


def run(kernel, shapes, args, scratch=(), flops=500000000):
    space = pl.BlockSpec(memory_space=pltpu.VMEM)
    moved = 4 * sum(int(np.prod(s)) for s in shapes)
    return pl.pallas_call(
        kernel,
        out_shape=[jax.ShapeDtypeStruct(s, F32) for s in shapes],
        in_specs=[space] * len(args),
        out_specs=[space] * len(shapes),
        scratch_shapes=[pltpu.VMEM(s, F32) for s in scratch],
        cost_estimate=pl.CostEstimate(flops=flops, bytes_accessed=moved, transcendentals=0),
        compiler_params=pltpu.CompilerParams(vmem_limit_bytes=16 << 20),
    )(*args)


def place_kernel(*refs):
    axes = (lax.axis_index("gx"), lax.axis_index("gy"), lax.axis_index("gz"))
    last_kernel(*refs, axes=axes)


def swapped(first, second, axis):
    count = lax.axis_size(axis)
    one = [(i, i ^ 1) for i in range(count)]
    two = [(i, (i + 1 if i % 2 else i - 1) % count) for i in range(count)]
    got = lax.ppermute(first, axis, one)
    return got, lax.ppermute(second, axis, two)


def everyone(array, axis):
    return lax.all_to_all(array, axis, 0, 0, tiled=True)


def steps(density, potential):
    tables = [jnp.asarray(t) for t in coarse_tables()]
    (own,) = run(part_kernel, [(6, 6, 8, LANES)], [density, potential], [(192, LANES)] * 2)
    xs = swapped(own, own, "gx")
    (shares,) = run(
        share_kernel,
        [(GX * GZ, 1, LANES)],
        [own],
        [(96, 16, LANES), (48, 16, LANES), (20, 24, LANES), (12, 24, LANES), (LANES, LANES)],
    )
    (plane,) = run(along_xz_kernel, [(GY, 2, LANES)], [everyone(shares, ("gx", "gz"))])
    blocks = everyone(plane, "gy")
    ys = swapped(*run(rim_y_kernel, [(6, 18, 4, LANES)] * 2, [own, *xs]), "gy")
    zs = swapped(*run(rim_z_kernel, [(27, 16, LANES)] * 2, [own, *xs, *ys]), "gz")
    level, fine, kept = run(
        fine_kernel,
        [(12, 16, LANES), (8, 10, 16, LANES), (8, 10, 16, LANES)],
        [own, *xs, *ys, *zs],
        [(144, 16, LANES), (144, 16, LANES)],
    )
    ys = swapped(level, level, "gy")
    wide, xa, xb = run(
        level_y_kernel, [(12, 32, LANES), (9, 32, LANES), (9, 32, LANES)], [level, *ys]
    )
    xs = swapped(xa, xb, "gx")
    level, mid = run(
        mid_kernel, [(24, 32, LANES), (18, 32, LANES)], [wide, *xs], [(24, 32, LANES)]
    )
    (out,) = run(
        place_kernel,
        [(12, 16, LANES)],
        [blocks, *tables, level, mid, fine, kept],
        [(18, 32, LANES), (80, 16, LANES), (192, LANES)],
    )
    return out


def solution(mesh):
    spec = P("gx", "gy", "gz")
    return jax.shard_map(steps, mesh=mesh, in_specs=(spec, spec), out_specs=spec, check_vma=False)
```

```python
import jax
import jax.numpy as jnp
import numpy as np
from jax import lax
from jax.experimental import pallas as pl
from jax.experimental.pallas import tpu as pltpu
from jax.sharding import PartitionSpec as P


GX, GY, GZ = 8, 16, 8
BX, BY, BZ = 6, 8, 64
LANES = 128
SHIFT = 4.25
SIXTH = 1.0 / 6.0
HI = lax.Precision.HIGHEST
F32 = jnp.float32


def roll(x, shift, axis):
    return pltpu.roll(x, shift % x.shape[axis], axis)


def iota(shape, dim):
    return lax.broadcasted_iota(jnp.int32, shape, dim)


def dot(a, b):
    return lax.dot_general(a, b, (((1,), (0,)), ((), ())), precision=HI, preferred_element_type=F32)


def dot_nt(a, b):
    return lax.dot_general(a, b, (((1,), (1,)), ((), ())), precision=HI, preferred_element_type=F32)


def plus(a, b):
    if a is None:
        return b
    return a if b is None else a + b


def basis_of(count):
    rows = np.arange(count)[:, None]
    cols = np.arange(count)[None, :]
    freq = (cols + 1) // 2
    angle = 2.0 * np.pi * freq * rows / count
    table = np.where(cols % 2 == 1, np.cos(angle), np.sin(angle)) * np.sqrt(2.0 / count)
    table = np.where(2 * freq == count, np.cos(angle) / np.sqrt(count), table)
    table = np.where(cols == 0, 1.0 / np.sqrt(count), table)
    modes = (np.arange(count) + 1) // 2
    return table, 2.0 - 2.0 * np.cos(2.0 * np.pi * modes / count)


def coarse_tables():
    qx, lx = basis_of(GX)
    qy, ly = basis_of(GY)
    qz, lz = basis_of(GZ)
    count = GX * GZ
    qxz = np.zeros((LANES, LANES))
    qxz[:count, :count] = np.einsum("ia,kc->ikac", qx, qz).reshape(count, count)
    lam = BX * BZ * ly[:, None, None] + BY * BZ * lx[None, :, None] + BX * BY * lz[None, None, :]
    lam[0, 0, 0] = 1.0
    table = -1.0 / lam
    table[0, 0, 0] = 0.0
    inverse = np.zeros((GY, LANES))
    inverse[:, :count] = table.reshape(GY, count)
    around = lambda n: np.arange(-1, n + 1) % n
    ty = np.repeat(qy[around(GY)][:, :, None], LANES, axis=2)
    tx = np.zeros((GX + 2, LANES))
    tx[:, :count] = np.repeat(qx[around(GX)], GZ, axis=1)
    tz = np.zeros((GZ + 2, LANES))
    tz[:, :count] = np.tile(qz[around(GZ)], (1, GX))
    return [np.asarray(t, np.float32) for t in (qxz, inverse, tx, ty, tz)]


def parting():
    rows, cols = iota((LANES, LANES), 0), iota((LANES, LANES), 1)
    return jnp.where(cols == (rows % 2) * 64 + rows // 2, 1.0, 0.0)


def unit_response():
    red = black = 0.0
    for _ in range(2):
        red = (6 * black - 1) / 6
        black = (6 * red - 1) / 6
    level = 0.5 * (4 * (1 - (6 * black - 6 * red)) + 4 * (1 - (6 * red - 6 * black)))
    one = [0.0, 0.0]
    for _ in range(4):
        one[0] = (6 * one[1] - level) / 6
        one[1] = (6 * one[0] - level) / 6
    v = [[own + group for own in (red, black)] for group in one]
    for _ in range(2):
        for own in (0, 1):
            near = 3 * (v[0][1 - own] + v[1][1 - own])
            v[0][own] = v[1][own] = (near - 1) / 6
    return v


CELLS = [(a, b, c) for a in (0, 1) for b in (0, 1) for c in (0, 1)]


def spread(depth, a, count):
    low = -((depth + a) // 2)
    high = (2 * count + depth - 1 - a) // 2
    return range(low, high + 1)


def beside(field, cell, x):
    a, b, c = cell
    total = plus(field.get(((1 - a, b, c), x)), field.get(((1 - a, b, c), x + (1 if a else -1))))
    other = field.get(((a, 1 - b, c), x))
    if other is not None:
        total = plus(total, other + roll(other, -1 if b else 1, 0))
    other = field.get(((a, b, 1 - c), x))
    if other is not None:
        total = plus(total, other + roll(other, -1 if c else 1, 1))
    return total


class Kept:
    def __init__(self, ref):
        self.ref = ref
        self.slots = {}

    def get(self, key):
        slot = self.slots.get(key)
        return None if slot is None else self.ref[slot]

    def put(self, key, value):
        slot = self.slots.setdefault(key, len(self.slots))
        self.ref[slot] = value


def fine_half(field, source, colour, depth):
    for cell in CELLS:
        if sum(cell) % 2 != colour:
            continue
        for x in spread(depth, cell[0], BX):
            near = beside(field, cell, x)
            s = source.get((cell, x))
            if near is None and s is None:
                continue
            value = near if s is None else (-s if near is None else near - s)
            field.put((cell, x), value * SIXTH)


def coarsened(field, source, x):
    total = None
    for cell in CELLS:
        if sum(cell) % 2 != 0:
            continue
        near = beside(field, cell, x)
        s = source.get((cell, x))
        own = field.get((cell, x))
        part = None if own is None else 6.0 * own
        part = plus(part, s)
        if near is not None:
            part = -near if part is None else part - near
        total = plus(total, part)
    return None if total is None else total * 0.5


def red_of(shape, x):
    return (iota(shape, 0) + iota(shape, 1) + (x % 2)) % 2 == 0


def beside_one(field, x):
    total = plus(field.get(x - 1), field.get(x + 1))
    own = field.get(x)
    if own is not None:
        total = plus(total, roll(own, 1, 0) + roll(own, -1, 0))
        total = total + (roll(own, 1, 1) + roll(own, -1, 1))
    return total


def one_half(field, source, colour, low, high, masks):
    for x in range(low, high):
        near = beside_one(field, x)
        s = source.get(x)
        own = field.get(x)
        if near is None and s is None:
            continue
        value = near if s is None else (-s if near is None else near - s)
        value = value * SIXTH
        red = masks[x % 2]
        rest = jnp.zeros_like(value) if own is None else own
        field.put(x, jnp.where(red, value, rest) if colour == 0 else jnp.where(red, rest, value))


def part_kernel(density, potential, out, dscratch, pscratch):
    t = parting()
    dscratch[...] = dot(density[...].reshape(192, LANES) - SHIFT, t)
    pscratch[...] = dot(potential[...].reshape(192, LANES), t)
    low = iota((BY, LANES), 1) < 64
    for x in range(BX):
        for a in (0, 1):
            rows = []
            for b in (0, 1):
                at = pl.ds((2 * x + a) * 16 + b, BY, stride=2)
                out[2 * a + b, x] = dscratch[at, :]
                rows.append(pscratch[at, :])
            out[4 + a, x] = jnp.where(low, rows[1 - a], rows[a])


def source_slot(cell):
    return 2 * cell[0] + cell[1]


def halves(cell):
    return 4 + cell[0], cell[2]


def share_kernel(pairs, out, fref, sref, eref, lref, stack):
    own = iota((BY, LANES), 1) < 64
    source, field = Kept(sref), Kept(fref)
    nothing = jnp.zeros((BY, LANES), F32)
    mass = None
    for cell in CELLS:
        for x in range(BX):
            value = pairs[source_slot(cell), x]
            mass = plus(mass, value) if cell[2] == 0 else mass
            if cell[2]:
                value = roll(value, 64, 1)
            source.put((cell, x), jnp.concatenate([jnp.where(own, value, 0.0), nothing], 0))
            if sum(cell) % 2:
                array, half = halves(cell)
                value = pairs[array, x]
                if half:
                    value = roll(value, 64, 1)
                field.put((cell, x), jnp.concatenate([jnp.where(own, value, 0.0), nothing], 0))
    for step in range(4):
        fine_half(field, source, step % 2, step + 1)
    level, error = Kept(lref), Kept(eref)
    near = iota((BY, LANES), 0) < 4
    for x in range(-3, BX + 3):
        value = coarsened(field, source, x)
        top, rim = value[:BY], value[BY:]
        level.put(x, jnp.concatenate([top, jnp.where(near, rim, 0.0), jnp.where(near, 0.0, rim)], 0))
    masks = [red_of((24, LANES), x) for x in (0, 1)]
    for step in range(4):
        one_half(error, level, step % 2, -3 - step, BX + 3 + step, masks)
    for i, (low, high) in enumerate(((-7, -6), (-6, 0), (0, 6), (6, 12), (12, 13))):
        total = None
        for x in range(low, high):
            part = plus(level.get(x), None if error.get(x) is None else 6.0 * error.get(x))
            around = beside_one(error, x)
            part = -around if part is None else part - around
            total = plus(total, jnp.where(masks[x % 2], part, 0.0))
        for j in range(3):
            stack[pl.ds((3 * i + j) * 8, 8), :] = total[8 * j : 8 * j + 8]
    stack[pl.ds(120, 8), :] = mass
    rows, cols = iota((LANES, LANES), 0), iota((LANES, LANES), 1)
    summed = dot(jnp.where(cols // 8 == rows, 1.0, 0.0), stack[...])
    row, lane = iota((8, LANES), 0), iota((8, LANES), 1)
    pick = ((row == 0) & (lane < 64)) | ((row == 1) & (lane >= 64) & (lane < 96))
    pick = pick | ((row == 2) & (lane >= 96))
    summed = jnp.where((rows == 15) & (cols < 64), summed + roll(summed, 64, 1), summed)
    summed = jnp.where((rows == 15) & (cols >= 64), 0.0, summed)
    sent = dot_nt(jnp.where(pick, 1.0, 0.0), summed)
    flat = sent[0:1] + roll(sent[1:2], 16, 1) + roll(sent[2:3], 32, 1)
    for peer in range(GX * GZ):
        out[peer] = flat


def along_xz_kernel(got, out):
    values = got[:, 0, :]
    lane = iota((GZ, LANES), 1)
    part, slot = lane // 16, lane % 16
    lines = []
    for i in range(GX):
        line = values[GZ * i : GZ * i + GZ]
        total = jnp.where(part == 0, line, 0.0)
        total = total + roll(jnp.where(part == 1, line, 0.0), 1, 0)
        lines.append(total + roll(jnp.where(part == 2, line, 0.0), -1, 0))
    rows = []
    for i in range(GX):
        total = jnp.where(slot == 15, lines[i], 0.0)
        for r in range(5):
            total = jnp.where((slot < 15) & (slot // 3 == r), lines[(i - (r - 2)) % GX], total)
        rows.append(total)
    total = jnp.concatenate(rows + rows, 0)
    row, col = iota((8, LANES), 0), iota((8, LANES), 1)
    take = (col < 48) & (col % 16 < 15) & ((col % 16) % 3 == row)
    take = take | ((row == 3) & (col == 15))
    sums = dot_nt(jnp.where(take, 1.0, 0.0), total)
    first = iota((1, LANES), 1) < 64
    sent = [jnp.where(first, sums[0:1], sums[1:2]), jnp.where(first, sums[2:3], sums[3:4])]
    sent = jnp.concatenate(sent, 0)
    for peer in range(GY):
        out[peer] = sent


def sides(axis, first, second):
    odd = lax.axis_index(axis) % 2 == 1

    def pick(swap):
        return lambda *at: jnp.where(odd != swap, first[at], second[at])

    return pick(False), pick(True)


def for_swaps(axis, low, high):
    odd = lax.axis_index(axis) % 2 == 1
    return jnp.where(odd, low, high), jnp.where(odd, high, low)


def wide_x(own, left, right, array, x):
    if x < 0:
        return left(array, x + BX)
    if x >= BX:
        return right(array, x - BX)
    return own[array, x]


def rim_y_kernel(own, xa, xb, ya, yb):
    left, right = sides("gx", xa, xb)
    for array in range(6):
        for x in range(-BX, 2 * BX):
            value = wide_x(own, left, right, array, x)
            ya[array, x + BX], yb[array, x + BX] = for_swaps("gy", value[:4], value[4:])


def tall(own, left, right, below, above, array, x):
    value = wide_x(own, left, right, array, x)
    rim = jnp.concatenate([above(array, x + BX), below(array, x + BX)], 0)
    return jnp.concatenate([value, rim], 0)


def groups():
    made = []
    for x in range(-BX, 2 * BX):
        made.append((x + BX, [(i, x) for i in range(4)]))
    for x in range(-BX, 3):
        made.append((18 + x + BX, [(4, x), (5, x), (4, x + 9), (5, x + 9)]))
    return made


def rim_z_kernel(own, xa, xb, ya, yb, za, zb):
    left, right = sides("gx", xa, xb)
    below, above = sides("gy", ya, yb)
    lane = iota((16, LANES), 1)
    for slot, members in groups():
        lows = highs = None
        for i, (array, x) in enumerate(members):
            value = tall(own, left, right, below, above, array, x)
            down = roll(value, 16 * i, 1)
            up = roll(value, 16 * (i + 1), 1)
            lows = down if lows is None else jnp.where((lane % 64) // 16 == i, down, lows)
            highs = up if highs is None else jnp.where((lane % 64) // 16 == i, up, highs)
        za[slot], zb[slot] = for_swaps("gz", lows, highs)


def fine_kernel(own, xa, xb, ya, yb, za, zb, level, rows, fine, kept, fref, sref):
    left, right = sides("gx", xa, xb)
    below, above = sides("gy", ya, yb)
    before, after = sides("gz", za, zb)
    source, field = Kept(sref), Kept(fref)
    lane = iota((16, LANES), 1)
    for slot, members in groups():
        up, down = after(slot), before(slot)
        for i, (array, x) in enumerate(members):
            value = tall(own, left, right, below, above, array, x)
            for c in (0, 1):
                mine = roll(value, 64, 1) if c else value
                right_rim = roll(up, 64 - 16 * i - 64 * c, 1)
                left_rim = roll(down, 48 - 16 * i + 64 * c, 1)
                full = jnp.where(lane < 64, mine, 0.0)
                full = jnp.where((lane >= 64) & (lane < 80), right_rim, full)
                full = jnp.where(lane >= 112, left_rim, full)
                if array < 4:
                    source.put(((array // 2, array % 2, c), x), full)
                else:
                    a = array - 4
                    b = (1 + a + c) % 2
                    field.put(((a, b, c), x), full)
    for step, depth in enumerate((10, 9, 8, 7)):
        fine_half(field, source, step % 2, depth)
    for x in range(12):
        value = coarsened(field, source, x - 3)
        level[x] = value
        rows[x] = value[:8]
        for at, row in ((x, 8), (12 + x, 15)):
            rows[12 + at // 8, pl.ds(at % 8, 1), :] = value[row : row + 1]
    for n, cell in enumerate(CELLS):
        for x in range(-2, BX + 2):
            fine[n, x + 2] = field.get((cell, x))
            kept[n, x + 2] = source.get((cell, x))


TILES = {k: 4 if k == 1 else 3 if k < 6 else 2 for k in range(1, 10)}
FIRST = {k: sum(TILES[i] for i in range(1, k)) for k in TILES}


def layer_tiles(value, k):
    near = iota((8, LANES), 0) < 4
    if TILES[k] == 4:
        return [value[8 * i : 8 * i + 8] for i in range(4)]
    if TILES[k] == 3:
        return [value[:8], value[8:16], value[24:]]
    return [value[:8], jnp.where(near, value[8:16], value[24:])]


def tiled_layer(tiles, k):
    near = iota((8, LANES), 0) < 4
    nothing = jnp.zeros((8, LANES), F32)
    got = [tiles(FIRST[k] + i) for i in range(TILES[k])]
    if TILES[k] == 3:
        got = [got[0], got[1], nothing, got[2]]
    if TILES[k] == 2:
        got = [got[0], jnp.where(near, got[1], 0.0), nothing, jnp.where(near, 0.0, got[1])]
    return jnp.concatenate(got, 0)


def level_y_kernel(own, ya, yb, wide, xa, xb):
    below, above = sides("gy", ya, yb)
    first = iota((8, LANES), 0) == 0
    last = iota((8, LANES), 0) == 7
    for x in range(12):
        tail = above(12 + x // 8)[x % 8 : x % 8 + 1]
        at = 12 + x
        lead = below(12 + at // 8)[at % 8 : at % 8 + 1]
        outer = jnp.where(first, tail, jnp.where(last, lead, 0.0))
        wide[x] = jnp.concatenate([own[x][:8], above(x), outer, below(x)], 0)
    for k in TILES:
        pairs = zip(layer_tiles(wide[k + 2], k), layer_tiles(wide[9 - k], k))
        for i, (low, high) in enumerate(pairs):
            xa[FIRST[k] + i], xb[FIRST[k] + i] = for_swaps("gx", low, high)


def mid_kernel(wide, xa, xb, level, mid, eref):
    left, right = sides("gx", xa, xb)
    for x in range(-9, BX + 9):
        if x < 0:
            value = tiled_layer(left, -x)
        elif x >= BX:
            value = tiled_layer(right, x - BX + 1)
        else:
            value = wide[x + 3]
        level[x + 9] = value
    source = Given(level, 9, 24)
    error = Kept(eref)
    masks = [red_of((32, LANES), x) for x in (0, 1)]
    for step, depth in enumerate((9, 8, 7, 6)):
        one_half(error, source, step % 2, -depth, BX + depth, masks)
    for x in range(-6, BX + 6):
        mid[x + 6] = error.get(x)


class Given:
    def __init__(self, ref, start, count):
        self.ref, self.start, self.count = ref, start, count

    def get(self, x):
        return self.ref[x + self.start] if 0 <= x + self.start < self.count else None

    def put(self, x, value):
        self.ref[x + self.start] = value


def solve_kernel(got, qxz, inverse, tx, ty, tz, coarse, constant):
    one, two = got[:, 0, :], got[:, 1, :]
    blocks = one + roll(roll(one, 64, 1), 1, 0) + roll(two, -1, 0)
    inside = iota((GY, LANES), 1) < GX * GZ
    mean = jnp.sum(jnp.where(inside, 0.0, two), keepdims=True)
    mean = mean * (1.0 / (GX * GY * GZ * 8 * BX * BY * BZ))
    blocks = jnp.where(inside, blocks, 0.0)
    level_out = jnp.sum(blocks, keepdims=True) * (1.0 / (GX * GY * GZ))
    blocks = jnp.where(inside, blocks - level_out, 0.0)
    half = dot(blocks, qxz[...])
    modes = None
    for y in range(GY):
        modes = plus(modes, half[y : y + 1, :] * ty[y + 1])
    modes = modes * inverse[...]
    ix, iy, iz = (lax.axis_index(axis) for axis in ("gx", "gy", "gz"))
    own_lane = iota((LANES, LANES), 0)
    zrow = lambda d: tz[pl.ds(iz + 1 + d, 1), :]
    spread_z = jnp.where(own_lane < 64, zrow(0), jnp.where(own_lane < 96, zrow(1), zrow(-1)))
    place = iota((16, LANES), 0)
    stacked = jnp.zeros((16, LANES), F32)
    for dy in (-1, 0, 1):
        line = jnp.sum(modes * ty[iy + 1 + dy], axis=0, keepdims=True)
        for dx in (-1, 0, 1):
            both = line * tx[pl.ds(ix + 1 + dx, 1), :]
            stacked = jnp.where(place == 3 * (dx + 1) + dy + 1, both, stacked)
    coarse[...] = dot_nt(stacked, spread_z)
    constant[...] = jnp.broadcast_to(mean, (8, LANES))


def place_kernel(solved, constant, level, mid, fine, kept, out, eref, fref, oref):
    coarse, mean = solved[...], constant[...]
    row = iota((32, LANES), 0)
    error = Given(eref, 6, 18)
    for dx in (-1, 0, 1):
        r = 3 * (dx + 1)
        add = jnp.where(row < 8, coarse[r + 1 : r + 2], jnp.where(row < 16, coarse[r + 2 : r + 3], coarse[r : r + 1]))
        for x in range(BX * dx, BX * dx + BX):
            error.put(x, mid[x + 6] + add)
    source = Given(level, 9, 24)
    masks = [red_of((32, LANES), x) for x in (0, 1)]
    for step, depth in enumerate((5, 4, 3, 2)):
        one_half(error, source, step % 2, -depth, BX + depth, masks)
    near = iota((8, LANES), 0) < 4
    field, terms = Kept(fref), Sources(kept)
    for x in range(-2, BX + 2):
        e = error.get(x)
        e = jnp.concatenate([e[:8], jnp.where(near, e[8:16], e[24:])], 0)
        for n, cell in enumerate(CELLS):
            field.put((cell, x), fine[n, x + 2] + e)
    for step, depth in enumerate((3, 2, 1, 0)):
        fine_half(field, terms, step % 2, depth)
    v = unit_response()
    shape = (8, LANES)
    lane = iota(shape, 1)
    for x in range(BX):
        group = (iota(shape, 0) + lane + x) % 2 == 0
        for a in (0, 1):
            for b in (0, 1):
                pair = []
                for c in (0, 1):
                    own = (a + b + c) % 2
                    value = field.get(((a, b, c), x))[:8]
                    pair.append(value - mean * jnp.where(group, v[0][own], v[1][own]))
                both = jnp.where(lane < 64, pair[0], roll(pair[1], 64, 1))
                oref[pl.ds((2 * x + a) * 16 + b, 8, stride=2), :] = both
    out[...] = dot_nt(oref[...], parting()).reshape(12, 16, LANES)


class Sources:
    def __init__(self, ref):
        self.ref = ref

    def get(self, key):
        cell, x = key
        return self.ref[CELLS.index(cell), x + 2] if -2 <= x < BX + 2 else None


def run(kernel, shapes, args, scratch=(), flops=500000000):
    space = pl.BlockSpec(memory_space=pltpu.VMEM)
    moved = 4 * sum(int(np.prod(s)) for s in shapes)
    return pl.pallas_call(
        kernel,
        out_shape=[jax.ShapeDtypeStruct(s, F32) for s in shapes],
        in_specs=[space] * len(args),
        out_specs=[space] * len(shapes),
        scratch_shapes=[pltpu.VMEM(s, F32) for s in scratch],
        cost_estimate=pl.CostEstimate(flops=flops, bytes_accessed=moved, transcendentals=0),
        compiler_params=pltpu.CompilerParams(vmem_limit_bytes=16 << 20),
    )(*args)


def swapped(first, second, axis):
    count = lax.axis_size(axis)
    one = [(i, i ^ 1) for i in range(count)]
    two = [(i, (i + 1 if i % 2 else i - 1) % count) for i in range(count)]
    got = lax.ppermute(first, axis, one)
    return got, lax.ppermute(second, axis, two)


def everyone(array, axis):
    return lax.all_to_all(array, axis, 0, 0, tiled=True)


def steps(density, potential):
    tables = [jnp.asarray(t) for t in coarse_tables()]
    (own,) = run(part_kernel, [(6, 6, 8, LANES)], [density, potential], [(192, LANES)] * 2)
    xs = swapped(own, own, "gx")
    (shares,) = run(
        share_kernel,
        [(GX * GZ, 1, LANES)],
        [own],
        [(96, 16, LANES), (48, 16, LANES), (20, 24, LANES), (12, 24, LANES), (LANES, LANES)],
    )
    (plane,) = run(along_xz_kernel, [(GY, 2, LANES)], [everyone(shares, ("gx", "gz"))])
    blocks = everyone(plane, "gy")
    ys = swapped(*run(rim_y_kernel, [(6, 18, 4, LANES)] * 2, [own, *xs]), "gy")
    zs = swapped(*run(rim_z_kernel, [(27, 16, LANES)] * 2, [own, *xs, *ys]), "gz")
    level, rows, fine, kept = run(
        fine_kernel,
        [(12, 16, LANES), (15, 8, LANES), (8, 10, 16, LANES), (8, 10, 16, LANES)],
        [own, *xs, *ys, *zs],
        [(144, 16, LANES), (144, 16, LANES)],
    )
    ys = swapped(rows, rows, "gy")
    wide, xa, xb = run(
        level_y_kernel, [(12, 32, LANES), (24, 8, LANES), (24, 8, LANES)], [level, *ys]
    )
    xs = swapped(xa, xb, "gx")
    level, mid = run(
        mid_kernel, [(24, 32, LANES), (18, 32, LANES)], [wide, *xs], [(24, 32, LANES)]
    )
    solved = run(solve_kernel, [(16, LANES), (8, LANES)], [blocks, *tables])
    (out,) = run(
        place_kernel,
        [(12, 16, LANES)],
        [*solved, level, mid, fine, kept],
        [(18, 32, LANES), (80, 16, LANES), (192, LANES)],
    )
    return out


def solution(mesh):
    spec = P("gx", "gy", "gz")
    return jax.shard_map(steps, mesh=mesh, in_specs=(spec, spec), out_specs=spec, check_vma=False)
```

```python
import functools

import jax
import jax.numpy as jnp
import numpy as np
from jax import lax
from jax.experimental import pallas as pl
from jax.experimental.pallas import tpu as pltpu
from jax.sharding import PartitionSpec as P


GX, GY, GZ = 8, 16, 8
BX, BY, BZ = 6, 8, 64
LANES = 128
SHIFT = 4.25
SIXTH = 1.0 / 6.0
HI = lax.Precision.HIGHEST
F32 = jnp.float32


def roll(x, shift, axis):
    return pltpu.roll(x, shift % x.shape[axis], axis)


def iota(shape, dim):
    return lax.broadcasted_iota(jnp.int32, shape, dim)


def dot(a, b):
    return lax.dot_general(a, b, (((1,), (0,)), ((), ())), precision=HI, preferred_element_type=F32)


def dot_nt(a, b):
    return lax.dot_general(a, b, (((1,), (1,)), ((), ())), precision=HI, preferred_element_type=F32)


def plus(a, b):
    if a is None:
        return b
    return a if b is None else a + b


def basis_of(count):
    rows = np.arange(count)[:, None]
    cols = np.arange(count)[None, :]
    freq = (cols + 1) // 2
    angle = 2.0 * np.pi * freq * rows / count
    table = np.where(cols % 2 == 1, np.cos(angle), np.sin(angle)) * np.sqrt(2.0 / count)
    table = np.where(2 * freq == count, np.cos(angle) / np.sqrt(count), table)
    table = np.where(cols == 0, 1.0 / np.sqrt(count), table)
    modes = (np.arange(count) + 1) // 2
    return table, 2.0 - 2.0 * np.cos(2.0 * np.pi * modes / count)


def coarse_tables():
    qx, lx = basis_of(GX)
    qy, ly = basis_of(GY)
    qz, lz = basis_of(GZ)
    count = GX * GZ
    qxz = np.zeros((LANES, LANES))
    qxz[:count, :count] = np.einsum("ia,kc->ikac", qx, qz).reshape(count, count)
    lam = BX * BZ * ly[:, None, None] + BY * BZ * lx[None, :, None] + BX * BY * lz[None, None, :]
    lam[0, 0, 0] = 1.0
    table = -1.0 / lam
    table[0, 0, 0] = 0.0
    inverse = np.zeros((GY, LANES))
    inverse[:, :count] = table.reshape(GY, count)
    around = lambda n: np.arange(-1, n + 1) % n
    ty = np.repeat(qy[around(GY)][:, :, None], LANES, axis=2)
    tx = np.zeros((GX + 2, LANES))
    tx[:, :count] = np.repeat(qx[around(GX)], GZ, axis=1)
    tz = np.zeros((GZ + 2, LANES))
    tz[:, :count] = np.tile(qz[around(GZ)], (1, GX))
    return [np.asarray(t, np.float32) for t in (qxz, inverse, tx, ty, tz)]


def parting():
    rows, cols = iota((LANES, LANES), 0), iota((LANES, LANES), 1)
    return jnp.where(cols == (rows % 2) * 64 + rows // 2, 1.0, 0.0)


def unit_response():
    red = black = 0.0
    for _ in range(2):
        red = (6 * black - 1) / 6
        black = (6 * red - 1) / 6
    level = 0.5 * (4 * (1 - (6 * black - 6 * red)) + 4 * (1 - (6 * red - 6 * black)))
    one = [0.0, 0.0]
    for _ in range(4):
        one[0] = (6 * one[1] - level) / 6
        one[1] = (6 * one[0] - level) / 6
    v = [[own + group for own in (red, black)] for group in one]
    for _ in range(2):
        for own in (0, 1):
            near = 3 * (v[0][1 - own] + v[1][1 - own])
            v[0][own] = v[1][own] = (near - 1) / 6
    return v


CELLS = [(a, b, c) for a in (0, 1) for b in (0, 1) for c in (0, 1)]


def spread(depth, a, count):
    low = -((depth + a) // 2)
    high = (2 * count + depth - 1 - a) // 2
    return range(low, high + 1)


def beside(field, cell, x):
    a, b, c = cell
    total = plus(field.get(((1 - a, b, c), x)), field.get(((1 - a, b, c), x + (1 if a else -1))))
    other = field.get(((a, 1 - b, c), x))
    if other is not None:
        total = plus(total, other + roll(other, -1 if b else 1, 0))
    other = field.get(((a, b, 1 - c), x))
    if other is not None:
        total = plus(total, other + roll(other, -1 if c else 1, 1))
    return total


class Kept:
    def __init__(self, ref):
        self.ref = ref
        self.slots = {}

    def get(self, key):
        slot = self.slots.get(key)
        return None if slot is None else self.ref[slot]

    def put(self, key, value):
        slot = self.slots.setdefault(key, len(self.slots))
        self.ref[slot] = value


def fine_half(field, source, colour, depth):
    for cell in CELLS:
        if sum(cell) % 2 != colour:
            continue
        for x in spread(depth, cell[0], BX):
            near = beside(field, cell, x)
            s = source.get((cell, x))
            if near is None and s is None:
                continue
            value = near if s is None else (-s if near is None else near - s)
            field.put((cell, x), value * SIXTH)


def coarsened(field, source, x):
    total = None
    for cell in CELLS:
        if sum(cell) % 2 != 0:
            continue
        near = beside(field, cell, x)
        s = source.get((cell, x))
        own = field.get((cell, x))
        part = None if own is None else 6.0 * own
        part = plus(part, s)
        if near is not None:
            part = -near if part is None else part - near
        total = plus(total, part)
    return None if total is None else total * 0.5


def red_of(shape, x):
    return (iota(shape, 0) + iota(shape, 1) + (x % 2)) % 2 == 0


def beside_one(field, x):
    total = plus(field.get(x - 1), field.get(x + 1))
    own = field.get(x)
    if own is not None:
        total = plus(total, roll(own, 1, 0) + roll(own, -1, 0))
        total = total + (roll(own, 1, 1) + roll(own, -1, 1))
    return total


def one_half(field, source, colour, low, high, masks):
    for x in range(low, high):
        near = beside_one(field, x)
        s = source.get(x)
        own = field.get(x)
        if near is None and s is None:
            continue
        value = near if s is None else (-s if near is None else near - s)
        value = value * SIXTH
        red = masks[x % 2]
        rest = jnp.zeros_like(value) if own is None else own
        field.put(x, jnp.where(red, value, rest) if colour == 0 else jnp.where(red, rest, value))


def part_kernel(density, potential, out, dscratch, pscratch):
    t = parting()
    dscratch[...] = dot(density[...].reshape(192, LANES) - SHIFT, t)
    pscratch[...] = dot(potential[...].reshape(192, LANES), t)
    low = iota((BY, LANES), 1) < 64
    for x in range(BX):
        for a in (0, 1):
            rows = []
            for b in (0, 1):
                at = pl.ds((2 * x + a) * 16 + b, BY, stride=2)
                out[2 * a + b, x] = dscratch[at, :]
                rows.append(pscratch[at, :])
            out[4 + a, x] = jnp.where(low, rows[1 - a], rows[a])


def source_slot(cell):
    return 2 * cell[0] + cell[1]


def halves(cell):
    return 4 + cell[0], cell[2]


def spread_kernel(pairs, level, xa, xb, xxa, xxb, fref, sref):
    own = iota((BY, LANES), 1) < 64
    source, field = Kept(sref), Kept(fref)
    nothing = jnp.zeros((BY, LANES), F32)
    for cell in CELLS:
        for x in range(BX):
            value = pairs[source_slot(cell), x]
            if cell[2]:
                value = roll(value, 64, 1)
            source.put((cell, x), jnp.concatenate([jnp.where(own, value, 0.0), nothing], 0))
            if sum(cell) % 2:
                array, half = halves(cell)
                value = pairs[array, x]
                if half:
                    value = roll(value, 64, 1)
                field.put((cell, x), jnp.concatenate([jnp.where(own, value, 0.0), nothing], 0))
    for step in range(4):
        fine_half(field, source, step % 2, step + 1)
    for x in range(12):
        value = coarsened(field, source, x - 3)
        level[x] = value
        for t in (0, 1):
            xa[2 * x + t] = value[8 * t : 8 * t + 8]
            xb[2 * x + t] = value[8 * t : 8 * t + 8]
    for array in range(6):
        for q in range(4):
            at = 24 + 4 * array + q
            xa[at], xb[at] = for_swaps("gx", pairs[array, q], pairs[array, 2 + q])
    for x in range(6):
        low, high = level[x], level[x + 6]
        for t in (0, 1):
            rows = slice(8 * t, 8 * t + 8)
            xxa[2 * x + t], xxb[2 * x + t] = for_swaps("gx", low[rows], high[rows], 2)


def share_kernel(pairs, given, out, eref, lref, stack):
    mass = None
    for cell in CELLS:
        for x in range(BX):
            mass = plus(mass, pairs[source_slot(cell), x]) if cell[2] == 0 else mass
    level, error = Kept(lref), Kept(eref)
    near = iota((BY, LANES), 0) < 4
    for x in range(-3, BX + 3):
        value = given[x + 3]
        top, rim = value[:BY], value[BY:]
        level.put(x, jnp.concatenate([top, jnp.where(near, rim, 0.0), jnp.where(near, 0.0, rim)], 0))
    masks = [red_of((24, LANES), x) for x in (0, 1)]
    for step in range(4):
        one_half(error, level, step % 2, -3 - step, BX + 3 + step, masks)
    for i, (low, high) in enumerate(((-7, -6), (-6, 0), (0, 6), (6, 12), (12, 13))):
        total = None
        for x in range(low, high):
            part = plus(level.get(x), None if error.get(x) is None else 6.0 * error.get(x))
            around = beside_one(error, x)
            part = -around if part is None else part - around
            total = plus(total, jnp.where(masks[x % 2], part, 0.0))
        for j in range(3):
            stack[pl.ds((3 * i + j) * 8, 8), :] = total[8 * j : 8 * j + 8]
    stack[pl.ds(120, 8), :] = mass
    rows, cols = iota((LANES, LANES), 0), iota((LANES, LANES), 1)
    summed = dot(jnp.where(cols // 8 == rows, 1.0, 0.0), stack[...])
    row, lane = iota((8, LANES), 0), iota((8, LANES), 1)
    pick = ((row == 0) & (lane < 64)) | ((row == 1) & (lane >= 64) & (lane < 96))
    pick = pick | ((row == 2) & (lane >= 96))
    summed = jnp.where((rows == 15) & (cols < 64), summed + roll(summed, 64, 1), summed)
    summed = jnp.where((rows == 15) & (cols >= 64), 0.0, summed)
    sent = dot_nt(jnp.where(pick, 1.0, 0.0), summed)
    flat = sent[0:1] + roll(sent[1:2], 16, 1) + roll(sent[2:3], 32, 1)
    for peer in range(GY):
        out[peer] = flat


def along_y_kernel(got, out):
    values = got[:, 0, :]
    lane = iota((GY, LANES), 1)
    slot = lane % 16
    total = jnp.where((slot % 3 == 0) | (slot == 15), values, 0.0)
    total = total + roll(jnp.where(slot % 3 == 1, values, 0.0), 1, 0)
    total = total + roll(jnp.where(slot % 3 == 2, values, 0.0), -1, 0)
    rows, cols = iota((LANES, LANES), 0), iota((LANES, LANES), 1)
    kind = jnp.where(rows % 16 == 15, 15, (rows // 16) * 5 + (rows % 16) // 3)
    take = (rows < 48) & (cols % 16 == kind) & ((rows % 16 < 15) | (rows == 15))
    tiled = dot(total, jnp.where(take, 1.0, 0.0))
    picked = jnp.where(lane // 16 == iota((GY, LANES), 0) % 8, tiled, 0.0)
    sent = [jnp.sum(picked[8 * r : 8 * r + 8], axis=0, keepdims=True) for r in (0, 1)]
    sent = jnp.concatenate(sent, 0)
    for peer in range(GX * GZ):
        out[peer] = sent


def upper_half(axis, step):
    return (lax.axis_index(axis) // step) % 2 == 1


def sides(axis, first, second, step=1):
    odd = upper_half(axis, step)

    def pick(swap):
        return lambda *at: jnp.where(odd != swap, first[at], second[at])

    return pick(False), pick(True)


def for_swaps(axis, low, high, step=1):
    odd = upper_half(axis, step)
    return jnp.where(odd, low, high), jnp.where(odd, high, low)


RAW = range(-4, BX + 4)
FAR = {"up": (5, 6, 7, 0), "down": (7, 0, 1, 2)}


def lies(shape, rows):
    row = iota(shape, 0)
    return functools.reduce(lambda a, b: a | b, [row == r for r in rows])


def wide_raw(own, left, right, array, x):
    if x < 0:
        return left(24 + 4 * array + x + 4)
    if x >= BX:
        return right(24 + 4 * array + x - BX)
    return own[array, x]


def join_x_kernel(own, level, xa, xb, xxa, xxb, wide, ya, yb, yya, yyb):
    left, right = sides("gx", xa, xb)
    left2, right2 = sides("gx", xxa, xxb, 2)
    for x in range(-9, BX + 9):
        for t in (0, 1):
            value = level[x + 3, pl.ds(8 * t, 8), :] if -3 <= x < 9 else None
            if x < 3:
                value = plus(value, left(2 * (x + 9) + t))
            else:
                value = plus(value, right(2 * (x - 3) + t))
            if x < -3:
                value = value + left2(2 * (x + 9) + t)
            if x >= 9:
                value = value + right2(2 * (x - 9) + t)
            wide[x + 9, pl.ds(8 * t, 8), :] = value
            ya[2 * (x + 9) + t] = value
            yb[2 * (x + 9) + t] = value
    shape = (8, LANES)
    near = iota(shape, 0) < 4
    for array in range(6):
        for n in range(7):
            one = wide_raw(own, left, right, array, 2 * n - 4)
            two = wide_raw(own, left, right, array, 2 * n - 3)
            low = jnp.where(near, one, roll(two, 4, 0))
            high = jnp.where(near, roll(one, 4, 0), two)
            at = 48 + 7 * array + n
            ya[at], yb[at] = for_swaps("gy", low, high)
    first = iota(shape, 0) == 0
    last = iota(shape, 0) == 7
    kept = {side: lies(shape, FAR[side]) for side in FAR}
    for n in range(7):
        rows = [[wide[2 * n + 5 + m, pl.ds(8 * t, 8), :] for t in (0, 1)] for m in (0, 1)]
        low = [jnp.where(first, top, rim) for top, rim in rows]
        high = [jnp.where(last, top, rim) for top, rim in rows]
        low = jnp.where(kept["up"], low[0], roll(low[1], 4, 0))
        high = jnp.where(kept["down"], high[0], roll(high[1], 4, 0))
        yya[n], yyb[n] = for_swaps("gy", low, high, 2)


def raw_rim(below, above, array, x):
    n, odd = divmod(x + 4, 2)
    at = 48 + 7 * array + n
    near = iota((8, LANES), 0) < 4
    if odd:
        return jnp.where(near, roll(above(at), 4, 0), below(at))
    return jnp.where(near, above(at), roll(below(at), 4, 0))


def raw_items():
    items = [(array, x) for array in range(6) for x in RAW]
    return [items[16 * n : 16 * n + 16] for n in range(6)]


def join_y_kernel(own, xa, xb, wide, ya, yb, yya, yyb, tall, raw, za, zb):
    left, right = sides("gx", xa, xb)
    below, above = sides("gy", ya, yb)
    below2, above2 = sides("gy", yya, yyb, 2)
    shape = (8, LANES)
    row = iota(shape, 0)
    zero = jnp.zeros(shape, F32)
    for x in range(-9, BX + 9):
        at = x + 9
        mine = [wide[at, pl.ds(8 * t, 8), :] for t in (0, 1)]
        up = [above(2 * at + t) for t in (0, 1)]
        down = [below(2 * at + t) for t in (0, 1)]
        far_up = far_down = zero
        if x in RAW:
            n, odd = divmod(x + 4, 2)
            far_up, far_down = above2(n), below2(n)
            if odd:
                far_up, far_down = roll(far_up, 4, 0), roll(far_down, 4, 0)
        tiles = [
            mine[0] + jnp.where(row >= 5, up[1], jnp.where(row < 3, down[1], 0.0)),
            up[0] + jnp.where(row < 4, mine[1], jnp.where(row >= 5, far_up, 0.0)),
            jnp.where(row == 0, up[1] + far_up, jnp.where(row == 7, down[1] + far_down, 0.0)),
            down[0] + jnp.where(row >= 4, mine[1], jnp.where(row < 3, far_down, 0.0)),
        ]
        tall[at] = jnp.concatenate(tiles, 0)
    lane = iota((32, LANES), 1)
    for slot in range(3):
        low = high = None
        for g in range(8):
            value = tall[8 * slot + g]
            one, two = roll(value, 16 * g + 3, 1), roll(value, 16 * g - 55, 1)
            low = one if low is None else jnp.where(lane // 16 == g, one, low)
            high = two if high is None else jnp.where(lane // 16 == g, two, high)
        for t in range(4):
            rows = slice(8 * t, 8 * t + 8)
            za[4 * slot + t], zb[4 * slot + t] = for_swaps("gz", low[rows], high[rows])
    lane = iota((16, LANES), 1)
    for slot, items in enumerate(raw_items()):
        low = high = None
        for i, (array, x) in enumerate(items):
            body = [wide_raw(own, left, right, array, x), raw_rim(below, above, array, x)]
            value = jnp.concatenate(body, 0)
            raw[array, x + 4] = value
            one, two = roll(value, 4 * i, 1), roll(value, 4 * i + 4, 1)
            low = one if low is None else jnp.where((lane % 64) // 4 == i, one, low)
            high = two if high is None else jnp.where((lane % 64) // 4 == i, two, high)
        for t in (0, 1):
            rows = slice(8 * t, 8 * t + 8)
            at = 12 + 2 * slot + t
            za[at], zb[at] = for_swaps("gz", low[rows], high[rows])


def field_slot(cell, x):
    return CELLS.index(cell) * len(RAW) + x + 4


class Lattice:
    def __init__(self, ref):
        self.ref = ref

    def get(self, key):
        return self.ref[field_slot(*key)] if key[1] in RAW else None

    def put(self, key, value):
        self.ref[field_slot(*key)] = value


def fine_kernel(raw, za, zb, fine, kept):
    before, after = sides("gz", za, zb)
    source, field = Lattice(kept), Known(fine)
    lane = iota((16, LANES), 1)
    for slot, items in enumerate(raw_items()):
        pair = (12 + 2 * slot, 13 + 2 * slot)
        up = jnp.concatenate([after(at) for at in pair], 0)
        down = jnp.concatenate([before(at) for at in pair], 0)
        for i, (array, x) in enumerate(items):
            value = raw[array, x + 4]
            for c in (0, 1):
                mine = roll(value, 64, 1) if c else value
                full = jnp.where(lane < 64, mine, 0.0)
                full = jnp.where((lane >= 64) & (lane < 68), roll(up, 64 - 4 * i - 64 * c, 1), full)
                full = jnp.where(lane >= 124, roll(down, 60 - 4 * i + 64 * c, 1), full)
                if array < 4:
                    source.put(((array // 2, array % 2, c), x), full)
                else:
                    a = array - 4
                    field.put(((a, (1 + a + c) % 2, c), x), full)
    for step, depth in enumerate((7, 6, 5, 4)):
        fine_half(field, source, step % 2, depth)


class Known(Lattice):
    def __init__(self, ref):
        super().__init__(ref)
        self.put_keys = set()

    def get(self, key):
        return super().get(key) if key in self.put_keys else None

    def put(self, key, value):
        self.put_keys.add(key)
        super().put(key, value)


def mid_kernel(tall, za, zb, level, mid, eref):
    before, after = sides("gz", za, zb)
    lane = iota((32, LANES), 1)
    own = (lane < 67) | (lane >= 125)
    for slot in range(3):
        up = jnp.concatenate([after(4 * slot + t) for t in range(4)], 0)
        down = jnp.concatenate([before(4 * slot + t) for t in range(4)], 0)
        for g in range(8):
            value = jnp.where(own, tall[8 * slot + g], 0.0)
            value = value + jnp.where((lane >= 61) & (lane < 73), roll(up, 61 - 16 * g, 1), 0.0)
            value = value + jnp.where((lane < 3) | (lane >= 119), roll(down, 119 - 16 * g, 1), 0.0)
            level[8 * slot + g] = value
    source = Given(level, 9, 24)
    error = Kept(eref)
    masks = [red_of((32, LANES), x) for x in (0, 1)]
    for step, depth in enumerate((9, 8, 7, 6)):
        one_half(error, source, step % 2, -depth, BX + depth, masks)
    for x in range(-6, BX + 6):
        mid[x + 6] = error.get(x)


class Given:
    def __init__(self, ref, start, count):
        self.ref, self.start, self.count = ref, start, count

    def get(self, x):
        return self.ref[x + self.start] if 0 <= x + self.start < self.count else None

    def put(self, x, value):
        self.ref[x + self.start] = value


def solve_kernel(got, qxz, inverse, tx, ty, tz, coarse, constant):
    lane = iota((GZ, LANES), 1)
    kind = lane % 16
    row, col = iota((8, LANES), 0), iota((8, LANES), 1)
    pick = jnp.where((col // 16 == row) & (col % 16 < 15), 1.0, 0.0)
    halves_of, mean = [], 0.0
    for r in (0, 1):
        values = got[:, r, :]
        lines = []
        for i in range(GX):
            line = values[GZ * i : GZ * i + GZ]
            mean = mean + jnp.where(kind == 15, line, 0.0)
            total = jnp.where(kind // 5 == 0, line, 0.0)
            total = total + roll(jnp.where(kind // 5 == 1, line, 0.0), 1, 0)
            lines.append(total + roll(jnp.where(kind // 5 == 2, line, 0.0), -1, 0))
        rows = []
        for i in range(GX):
            total = lines[(i + 2) % GX]
            for d in range(1, 5):
                total = jnp.where(kind % 5 == d, lines[(i - (d - 2)) % GX], total)
            rows.append(total)
        halves_of.append(dot_nt(pick, jnp.concatenate(rows + rows, 0)))
    blocks = jnp.concatenate(halves_of, 0)
    inside = iota((GY, LANES), 1) < GX * GZ
    mean = jnp.sum(mean, keepdims=True) * (1.0 / (GX * GY * GZ * 8 * BX * BY * BZ))
    blocks = jnp.where(inside, blocks, 0.0)
    level_out = jnp.sum(blocks, keepdims=True) * (1.0 / (GX * GY * GZ))
    blocks = jnp.where(inside, blocks - level_out, 0.0)
    half = dot(blocks, qxz[...])
    modes = None
    for y in range(GY):
        modes = plus(modes, half[y : y + 1, :] * ty[y + 1])
    modes = modes * inverse[...]
    ix, iy, iz = (lax.axis_index(axis) for axis in ("gx", "gy", "gz"))
    own_lane = iota((LANES, LANES), 0)
    zrow = lambda d: tz[pl.ds(iz + 1 + d, 1), :]
    spread_z = jnp.where(own_lane < 64, zrow(0), jnp.where(own_lane < 96, zrow(1), zrow(-1)))
    place = iota((16, LANES), 0)
    stacked = jnp.zeros((16, LANES), F32)
    for dy in (-1, 0, 1):
        line = jnp.sum(modes * ty[iy + 1 + dy], axis=0, keepdims=True)
        for dx in (-1, 0, 1):
            both = line * tx[pl.ds(ix + 1 + dx, 1), :]
            stacked = jnp.where(place == 3 * (dx + 1) + dy + 1, both, stacked)
    coarse[...] = dot_nt(stacked, spread_z)
    constant[...] = jnp.broadcast_to(mean, (8, LANES))


def place_kernel(solved, constant, level, mid, fine, kept, out, eref, fref, oref):
    coarse, mean = solved[...], constant[...]
    row = iota((32, LANES), 0)
    error = Given(eref, 6, 18)
    for dx in (-1, 0, 1):
        r = 3 * (dx + 1)
        add = jnp.where(row < 8, coarse[r + 1 : r + 2], jnp.where(row < 16, coarse[r + 2 : r + 3], coarse[r : r + 1]))
        for x in range(BX * dx, BX * dx + BX):
            error.put(x, mid[x + 6] + add)
    source = Given(level, 9, 24)
    masks = [red_of((32, LANES), x) for x in (0, 1)]
    for step, depth in enumerate((5, 4, 3, 2)):
        one_half(error, source, step % 2, -depth, BX + depth, masks)
    near = iota((8, LANES), 0) < 4
    field, terms = Kept(fref), Lattice(kept)
    for x in range(-2, BX + 2):
        e = error.get(x)
        e = jnp.concatenate([e[:8], jnp.where(near, e[8:16], e[24:])], 0)
        for cell in CELLS:
            field.put((cell, x), fine[field_slot(cell, x)] + e)
    for step, depth in enumerate((3, 2, 1, 0)):
        fine_half(field, terms, step % 2, depth)
    v = unit_response()
    shape = (8, LANES)
    lane = iota(shape, 1)
    for x in range(BX):
        group = (iota(shape, 0) + lane + x) % 2 == 0
        for a in (0, 1):
            for b in (0, 1):
                pair = []
                for c in (0, 1):
                    own = (a + b + c) % 2
                    value = field.get(((a, b, c), x))[:8]
                    pair.append(value - mean * jnp.where(group, v[0][own], v[1][own]))
                both = jnp.where(lane < 64, pair[0], roll(pair[1], 64, 1))
                oref[pl.ds((2 * x + a) * 16 + b, 8, stride=2), :] = both
    out[...] = dot_nt(oref[...], parting()).reshape(12, 16, LANES)


def run(kernel, shapes, args, scratch=(), flops=500000000):
    space = pl.BlockSpec(memory_space=pltpu.VMEM)
    moved = 4 * sum(int(np.prod(s)) for s in shapes)
    return pl.pallas_call(
        kernel,
        out_shape=[jax.ShapeDtypeStruct(s, F32) for s in shapes],
        in_specs=[space] * len(args),
        out_specs=[space] * len(shapes),
        scratch_shapes=[pltpu.VMEM(s, F32) for s in scratch],
        cost_estimate=pl.CostEstimate(flops=flops, bytes_accessed=moved, transcendentals=0),
        compiler_params=pltpu.CompilerParams(vmem_limit_bytes=16 << 20),
    )(*args)


def swapped(first, second, axis, step=1):
    count = lax.axis_size(axis)
    one = [(i, i ^ step) for i in range(count)]
    two = [(i, (i + step if (i // step) % 2 else i - step) % count) for i in range(count)]
    got = lax.ppermute(first, axis, one)
    return got, lax.ppermute(second, axis, two)


def everyone(array, axis):
    return lax.all_to_all(array, axis, 0, 0, tiled=True)


def steps(density, potential):
    tables = [jnp.asarray(t) for t in coarse_tables()]
    (own,) = run(part_kernel, [(6, 6, 8, LANES)], [density, potential], [(192, LANES)] * 2)
    level, xa, xb, xxa, xxb = run(
        spread_kernel,
        [(12, 16, LANES), (48, 8, LANES), (48, 8, LANES), (12, 8, LANES), (12, 8, LANES)],
        [own],
        [(96, 16, LANES), (48, 16, LANES)],
    )
    xx = swapped(xxa, xxb, "gx", 2)
    xs = swapped(xa, xb, "gx")
    (share,) = run(
        share_kernel,
        [(GY, 1, LANES)],
        [own, level],
        [(20, 24, LANES), (12, 24, LANES), (LANES, LANES)],
    )
    (line,) = run(along_y_kernel, [(GX * GZ, 2, LANES)], [everyone(share, "gy")])
    blocks = everyone(line, ("gx", "gz"))
    wide, ya, yb, yya, yyb = run(
        join_x_kernel,
        [(24, 16, LANES), (90, 8, LANES), (90, 8, LANES), (7, 8, LANES), (7, 8, LANES)],
        [own, level, *xs, *xx],
    )
    yy = swapped(yya, yyb, "gy", 2)
    ys = swapped(ya, yb, "gy")
    tall, raw, za, zb = run(
        join_y_kernel,
        [(24, 32, LANES), (6, 14, 16, LANES), (24, 8, LANES), (24, 8, LANES)],
        [own, *xs, wide, *ys, *yy],
    )
    zs = swapped(za, zb, "gz")
    level, mid = run(
        mid_kernel, [(24, 32, LANES), (18, 32, LANES)], [tall, *zs], [(24, 32, LANES)]
    )
    fine, kept = run(fine_kernel, [(112, 16, LANES)] * 2, [raw, *zs])
    solved = run(solve_kernel, [(16, LANES), (8, LANES)], [blocks, *tables])
    (out,) = run(
        place_kernel,
        [(12, 16, LANES)],
        [*solved, level, mid, fine, kept],
        [(18, 32, LANES), (80, 16, LANES), (192, LANES)],
    )
    return out


def solution(mesh):
    spec = P("gx", "gy", "gz")
    return jax.shard_map(steps, mesh=mesh, in_specs=(spec, spec), out_specs=spec, check_vma=False)
```
